256 devices in a mesh: ka: 32 (over z_hi, y, core), freq: 8 (over z_lo, x).
Axes of the slice: x: 4, y: 4, z: 8 (z_hi: 4, z_lo: 2; z = z_hi * 2 + z_lo), core: 2. Of those that a mesh axis runs over, the one named last changes fastest.
Arguments:
- energy: float32 [32, 128], P('ka'), may hold values from -2.4 to 2.4, as said below
- projector: float32 [32, 2, 128, 40], P('ka'), may hold values from -0.25 to 0.25
- self_energy: float32 [128, 2, 40, 40], P('freq'), may hold values from -0.5 to 0.5
- multiplicity: int32 [32], P('ka'), may hold values from 1 to 5
- orbitals: float32 [32, 2, 128, 32, 1024], P('ka', None, None, None, 'freq'), may hold values from -12 to 12
- owner: int32 [32], replicated, may hold values from 0 to 31, each once
- rotation: float32 [40, 40], replicated, may hold values from -1 to 1
Outputs:
- local_green: float32 [128, 2, 40, 40], P('freq')
- slab_charge: float32 [32, 1024], P('ka', 'freq')
The draws below stay inside these ranges and needn't reach their ends.
Inputs may be any that keep to these rules, and one draw needn't show every extreme that they name: Every band energy has a magnitude between 1.6 and 2.4. `owner`: each ka index owns exactly one slab.
All inputs are finite; a program needn't handle non-finite values.
Results may differ from the reference program's by a relative error of at most 0.0001.
Values sent between devices are 32-bit elements; how exact they have to be, the bound alone decides.
No kernel may reach another device: no remote copies, remote signals or barrier semaphores. Data moves between devices by JAX's collectives and lax.ppermute only.
A program may use at most 64 MiB of HBM per device.

```python
import math
import jax
import jax.numpy as jnp
from jax import lax

NB = 128
NO = 40
F_DEV = 16
NS_STEPS = 3
KPTS = 32
FERMION_POLES = 128
SLABS = 32
SLAB_PTS = 1024


def draw_energy(key, part):
    sign_key, size_key = jax.random.split(jax.random.fold_in(key, 43))
    quarter = jax.random.randint(sign_key, (KPTS, NB), 0, 4)
    sign = jnp.where(quarter < 3, -1.0, 1.0).astype(jnp.float32)
    spread = jax.random.uniform(size_key, (KPTS, NB), jnp.float32, 0.0, 1.0)
    magnitude = 1.6 + 0.8 * spread
    return (sign * magnitude).astype(jnp.float32)


def draw_multiplicity(key, part):
    random_part = jax.random.randint(jax.random.fold_in(key, 11), (KPTS,), 1, 3)
    rising = 4 * jnp.arange(KPTS, dtype=jnp.int32) // KPTS
    return (random_part + rising).astype(jnp.int32)


def draw_self_energy(key, part):
    shift_key, damp_key, couple_key = jax.random.split(jax.random.fold_in(key, 29), 3)
    off_diagonal = 1.0 - jnp.eye(NO, dtype=jnp.float32)
    coupling = jax.random.truncated_normal(couple_key, -3.0, 3.0, (FERMION_POLES, 2, NO, NO), jnp.float32)
    damping = jnp.exp(jax.random.uniform(damp_key, (FERMION_POLES, NO), jnp.float32, math.log(0.05), math.log(0.5)))
    shifting = jax.random.uniform(shift_key, (FERMION_POLES, NO), jnp.float32, -0.4, 0.4)
    coupling = coupling * (0.12 / math.sqrt(NO)) * off_diagonal
    diagonal = jnp.stack([shifting, -damping], axis=1)[:, :, :, None] * jnp.eye(NO, dtype=jnp.float32)
    return (coupling + diagonal).astype(jnp.float32)


def steps_of(rng, dims, cuts, smallest, top_value):
    loudness, own = 1.0, jax.random.fold_in(rng, 6)
    for axis_at, shards_of in cuts:
        draws = jnp.exp(jax.random.uniform(jax.random.fold_in(own, axis_at), (shards_of,), jnp.float32, smallest / len(cuts), top_value / len(cuts)))
        loudness = loudness * jnp.repeat(draws, dims[axis_at] // shards_of).reshape([-1 if axis == axis_at else 1 for axis in range(len(dims))])
    return loudness


def gaussian(own_key, shape, scale, limit, pieces=(), held_as=jnp.bfloat16):
    drawn = scale * jax.random.normal(own_key, shape, jnp.float32)
    if pieces:
        drawn = drawn * steps_of(own_key, shape, pieces, -0.22, 0.18)
    return jnp.clip(drawn, -limit, limit).astype(held_as)


def setup_inputs(seed: int = 0) -> dict:
    key_list = jax.random.split(jax.random.key(seed), 8)
    return {
        "energy": draw_energy(jax.random.fold_in(key_list[7], 71), 0),
        "projector": gaussian(key_list[1], (KPTS, 2, NB, NO), (4 * NB) ** -0.5, 0.25, ((0, 32),), jnp.float32),
        "self_energy": draw_self_energy(jax.random.fold_in(key_list[7], 71), 0),
        "multiplicity": draw_multiplicity(jax.random.fold_in(key_list[7], 71), 0),
        "orbitals": gaussian(key_list[4], (KPTS, 2, NB, SLABS, SLAB_PTS), 2.0, 12.0, ((0, 32), (4, 8)), jnp.float32),
        "owner": jax.random.permutation(key_list[5], SLABS).astype(jnp.int32),
        "rotation": gaussian(key_list[6], (NO, NO), NO ** -0.5, 1.0, (), jnp.float32),
    }


PRECISE = lax.Precision.HIGHEST


def complex_product(first_pair, second_pair, formula):
    direct = jnp.einsum(formula, first_pair[0], second_pair[0], precision=PRECISE)
    opposed = jnp.einsum(formula, first_pair[1], second_pair[1], precision=PRECISE)
    mixed_one = jnp.einsum(formula, first_pair[0], second_pair[1], precision=PRECISE)
    mixed_two = jnp.einsum(formula, first_pair[1], second_pair[0], precision=PRECISE)
    return (direct - opposed, mixed_one + mixed_two)


def complex_times(first_pair, second_pair):
    return (first_pair[0] * second_pair[0] - first_pair[1] * second_pair[1],
            first_pair[0] * second_pair[1] + first_pair[1] * second_pair[0])


def green_block(energy_row, projector_pair, self_pair, pole_location):
    band_count = energy_row.shape[0]
    identity = jnp.eye(band_count, dtype=jnp.float32)
    squared = pole_location[:, None] * pole_location[:, None] + energy_row[None, :] * energy_row[None, :]
    bare_real = -energy_row[None, :] / squared
    bare_imag = -pole_location[:, None] / squared
    rightward_scale = (bare_real[:, None, :], bare_imag[:, None, :])
    row_side = (bare_real[:, :, None], bare_imag[:, :, None])
    adjoint = (projector_pair[0].T, -projector_pair[1].T)
    folded = complex_product(self_pair, adjoint, "fab,bj->faj")
    upfold = complex_product(projector_pair, folded, "ia,faj->fij")
    sandwich = complex_times(row_side, complex_times(upfold, rightward_scale))
    reciprocal_operator = (identity * rightward_scale[0] + sandwich[0], identity * rightward_scale[1] + sandwich[1])
    for repeat in range(NS_STEPS - 1):
        reduced = complex_product(adjoint, reciprocal_operator, "aj,fjk->fak")
        coupled = complex_product(self_pair, reduced, "fab,fbk->fak")
        lifted = complex_product(projector_pair, coupled, "ia,fak->fik")
        shift_real = -energy_row[None, :, None] * reciprocal_operator[0] - pole_location[:, None, None] * reciprocal_operator[1]
        shift_imag = -energy_row[None, :, None] * reciprocal_operator[1] + pole_location[:, None, None] * reciprocal_operator[0]
        residue = (identity - shift_real + lifted[0], lifted[1] - shift_imag)
        update = complex_product(reciprocal_operator, residue, "fij,fjk->fik")
        reciprocal_operator = (reciprocal_operator[0] + update[0], reciprocal_operator[1] + update[1])
    return reciprocal_operator, rightward_scale


def electron_filling(reciprocal_operator, rightward_scale, thermal_level):
    band_count = reciprocal_operator[0].shape[1]
    identity = jnp.eye(band_count, dtype=jnp.float32)
    excess_inphase = jnp.sum(reciprocal_operator[0] - identity * rightward_scale[0], axis=0)
    excess_quadrature = jnp.sum(reciprocal_operator[1] - identity * rightward_scale[1], axis=0)
    return (thermal_level * (excess_inphase + excess_inphase.T), thermal_level * (excess_quadrature - excess_quadrature.T))


def project_local(reciprocal_operator, projector_pair):
    adjoint = (projector_pair[0].T, -projector_pair[1].T)
    reduced = complex_product(adjoint, reciprocal_operator, "aj,fjk->fak")
    return complex_product(reduced, projector_pair, "fak,kb->fab")


def slab_density(orbital_filling_table, orbital_set):
    top_rows = jnp.concatenate([orbital_filling_table[0], -orbital_filling_table[1]], axis=1)
    bottom_rows = jnp.concatenate([orbital_filling_table[1], orbital_filling_table[0]], axis=1)
    realified = jnp.concatenate([top_rows, bottom_rows], axis=0)
    columns = orbital_set.reshape(realified.shape[0], -1)
    product = jnp.dot(realified, columns, precision=PRECISE, preferred_element_type=jnp.float32)
    return jnp.sum(columns * product, axis=0)


def reference(energy, projector, self_energy, multiplicity, orbitals, owner, rotation):
    thermal_level = 0.25 / FERMION_POLES
    slot_index = jnp.arange(FERMION_POLES, dtype=jnp.int32)
    fermionic_poles = (slot_index % F_DEV) * (FERMION_POLES // F_DEV) + slot_index // F_DEV
    pole_location = (2 * fermionic_poles + 1).astype(jnp.float32) * (math.pi * thermal_level)
    self_pair = (self_energy[:, 0], self_energy[:, 1])

    def accumulate(running, inputs):
        local_real, local_imag, charge = running
        energy_row, projector_one, multiple, orbital_set = inputs
        projector_pair = (projector_one[0], projector_one[1])
        reciprocal_operator, rightward_scale = green_block(energy_row, projector_pair, self_pair, pole_location)
        weight = multiple.astype(jnp.float32)
        projected = project_local(reciprocal_operator, projector_pair)
        orbital_filling_table = electron_filling(reciprocal_operator, rightward_scale, thermal_level)
        charge = charge + weight * slab_density(orbital_filling_table, orbital_set)
        return (local_real + weight * projected[0], local_imag + weight * projected[1], charge), None

    initial = (jnp.zeros((FERMION_POLES, NO, NO), jnp.float32), jnp.zeros((FERMION_POLES, NO, NO), jnp.float32),
               jnp.zeros((SLABS * SLAB_PTS,), jnp.float32))
    finals, unused = lax.scan(accumulate, initial, (energy, projector, multiplicity, orbitals))
    local_real, local_imag, charge = finals
    weight_total = jnp.sum(multiplicity.astype(jnp.float32))
    stacked = jnp.stack([local_real, local_imag]) / weight_total
    turned = jnp.einsum("pfbc,cd->pfbd", stacked, rotation, precision=PRECISE)
    rotated = jnp.einsum("ba,pfbd->pfad", rotation, turned, precision=PRECISE)
    local_green = jnp.transpose(rotated, (1, 0, 2, 3))
    slab_rows = charge.reshape(SLABS, SLAB_PTS) / weight_total
    selector = (owner[None, :] == jnp.arange(SLABS, dtype=jnp.int32)[:, None]).astype(jnp.float32)
    slab_charge = jnp.dot(selector, slab_rows, precision=PRECISE)
    return local_green, slab_charge
```

```python
import math

import jax
import jax.numpy as jnp
from jax import lax
from jax.experimental import pallas as pl
from jax.experimental.pallas import tpu as pltpu
from jax.sharding import PartitionSpec as P

F32 = jnp.float32
BF16 = jnp.bfloat16
LANES = 128
WIDE = 3
PIECE = 16


def low(x):
    return x - x.astype(BF16).astype(F32)


def mm(a, b):
    return jnp.dot(a, b, preferred_element_type=F32)


def mm3(a, b, b_low):
    rows = a.shape[0]
    both = mm(jnp.concatenate([a, low(a)], axis=0), b)
    return both[:rows] + both[rows:] + mm(a, b_low)


def blocks(wide, masks):
    n = wide.shape[0]
    rows = [jnp.where(m, wide, 0.0) for m in masks]
    rows.append(jnp.zeros((LANES - WIDE * n, LANES), F32))
    return jnp.concatenate(rows, axis=0)


def block_weights(wide, masks):
    def form(w):
        re = blocks(w[:, :LANES], masks)
        im = blocks(w[:, LANES:], masks)
        return jnp.concatenate(
            [jnp.concatenate([re, im], axis=1), jnp.concatenate([-im, re], axis=1)], axis=0
        )

    return form(wide), form(low(wide))


def green_kernel(pole_total, orbital_count, pole_stride, thermal_level):
    groups = -(-pole_total // WIDE)
    n = orbital_count

    def kernel(mult_ref, energy_ref, proj_ref, self_ref, rot_ref, dens_ref, rows_ref, flat_ref):
        weight = mult_ref[0].astype(F32)
        shift = lax.axis_index("freq")
        lane = lax.broadcasted_iota(jnp.int32, (n, LANES), 1)
        masks = [(lane >= n * j) & (lane < n * (j + 1)) for j in range(WIDE)]
        energy = energy_ref[...]
        pt = (proj_ref[0, 0], proj_ref[0, 1])
        step = math.pi * thermal_level

        def spread(x):
            tail = jnp.zeros((LANES - WIDE * n, LANES), F32)
            return jnp.concatenate([x] * WIDE + [tail], axis=0).T

        p3 = (spread(pt[0]), spread(pt[1]))
        energy_col = jnp.broadcast_to(energy, (LANES, LANES)).T
        rot = rot_ref[...]
        pt_both = jnp.concatenate([pt[0], pt[1]], axis=1)
        rot_t = rot.T
        turned = mm3(rot_t, pt_both, low(pt_both))
        left = jnp.concatenate([pt_both, turned], axis=0)
        rot_wide = jnp.concatenate([rot] * WIDE + [jnp.zeros((n, LANES - WIDE * n), F32)], axis=1)
        zero = jnp.zeros((LANES, LANES), F32)

        def rot_form(w):
            b = blocks(w, masks)
            return jnp.concatenate(
                [jnp.concatenate([b, zero], axis=1), jnp.concatenate([zero, b], axis=1)], axis=0
            )

        lane_row = lax.broadcasted_iota(jnp.int32, (1, LANES), 1)
        block_of = jnp.where(lane_row >= 2 * n, 2, jnp.where(lane_row >= n, 1, 0))

        gp = []
        for g in range(groups):
            slot = block_of + WIDE * g
            pole = (2 * (slot * pole_stride + shift) + 1).astype(F32) * step
            inv = 1.0 / (pole * pole + energy_col * energy_col)
            br = -energy_col * inv
            bi = -pole * inv
            gp.append((br * p3[0] - bi * p3[1], br * p3[1] + bi * p3[0]))

        big = []
        for g in range(groups):
            xr, xi = gp[g]

            def form(r, i):
                return jnp.concatenate(
                    [jnp.concatenate([r, i], axis=1), jnp.concatenate([i, -r], axis=1)], axis=0
                )

            big.append(mm3(left, form(xr, xi), form(low(xr), low(xi))))
        small = [b[:n] for b in big]
        stacked = jnp.concatenate(big, axis=0)
        right = mm3(stacked, rot_form(rot_wide), rot_form(low(rot_wide)))
        small_right = [right[2 * n * g : 2 * n * g + n] for g in range(groups)]
        both_right = [right[2 * n * g + n : 2 * n * (g + 1)] for g in range(groups)]

        sig = []
        pad = jnp.zeros((n, LANES - WIDE * n), F32)
        none = jnp.zeros((n, n), F32)
        for g in range(groups):
            halves = []
            for c in range(2):
                parts = []
                for j in range(WIDE):
                    q = WIDE * g + j
                    parts.append(self_ref[q, c] if q < pole_total else none)
                halves.append(jnp.concatenate(parts + [pad], axis=1))
            sig.append(jnp.concatenate(halves, axis=1))

        first = [mm3(big[g], *block_weights(sig[g], masks)) for g in range(groups)]
        a1 = [f[:n] for f in first]
        a1_left = [f[n:] for f in first]
        a2 = [mm3(a1[g], *block_weights(a1[g], masks)) for g in range(groups)]
        total = []
        for g in range(groups):
            w = block_weights(a2[g], masks)
            a34 = mm3(jnp.concatenate([a1[g], a2[g]], axis=0), *w)
            a34 = a34[:n] + a34[n:]
            total.append(a1[g] + a2[g] + a34 + mm3(a34, *w))
        last = [
            mm3(jnp.concatenate([sig[g], a1_left[g]], axis=0), *block_weights(total[g], masks))
            for g in range(groups)
        ]
        dress = [sig[g] + last[g][:n] for g in range(groups)]

        acc = None
        for g in range(groups):
            xr, xi = gp[g]
            w = mm3(jnp.concatenate([xr, xi], axis=1), *block_weights(dress[g], masks))
            res, ims = [], []
            for j in range(WIDE):
                q = WIDE * g + j
                pole = (2 * (q * pole_stride + shift) + 1).astype(F32) * step
                inv = 1.0 / (pole * pole + energy * energy)
                br = -energy * inv
                bi = -pole * inv
                res.append(pt[0] * br + pt[1] * bi)
                ims.append(pt[0] * bi - pt[1] * br)
            tail = jnp.zeros((LANES - WIDE * n, LANES), F32)
            re = jnp.concatenate(res + [tail], axis=0)
            im = jnp.concatenate(ims + [tail], axis=0)

            def form(r, i):
                return jnp.concatenate(
                    [jnp.concatenate([r, i], axis=1), jnp.concatenate([-i, r], axis=1)], axis=0
                )

            part = mm3(w, form(re, im), form(low(re), low(im)))
            acc = part if acc is None else acc + part
        er = acc[:, :LANES]
        ei = acc[:, LANES:]
        row = lax.broadcasted_iota(jnp.int32, (LANES, LANES), 0)
        col = lax.broadcasted_iota(jnp.int32, (LANES, LANES), 1)
        scale = weight * thermal_level
        dens_ref[...] = scale * jnp.where(row <= col, er + er.T, ei - ei.T)

        for g in range(groups):
            out = both_right[g] + mm3(
                a1_left[g] + last[g][n:], *block_weights(small_right[g], masks)
            )
            out = weight * out
            flat_ref[2 * n * g : 2 * n * g + n, :] = out[:, :LANES]
            flat_ref[2 * n * g + n : 2 * n * (g + 1), :] = out[:, LANES:]
        per = PIECE - 1
        for d in range(rows_ref.shape[0]):
            rows_ref[d, 0:per, :] = flat_ref[per * d : per * (d + 1), :]
            rows_ref[d, per:PIECE, :] = jnp.broadcast_to(weight, (1, LANES))

    return kernel


def split_kernel(orb_ref, high_ref, other_ref):
    bands = 2 * orb_ref.shape[2]
    slabs = orb_ref.shape[3]
    flat = orb_ref.reshape(bands * slabs, LANES)
    for s in range(slabs):
        x = flat[pl.ds(s, bands, stride=slabs), :]
        h = x.astype(BF16)
        high_ref[s] = h
        other_ref[s] = 2.0 * x - h.astype(F32)


def charge_kernel(owner_ref, dens_ref, local_ref, high_ref, other_ref, out_ref):
    packed = jnp.sum(dens_ref[...], axis=0)
    packed_t = packed.T
    row = lax.broadcasted_iota(jnp.int32, packed.shape, 0)
    col = lax.broadcasted_iota(jnp.int32, packed.shape, 1)
    re = jnp.where(row <= col, packed, packed_t)
    im = jnp.where(row > col, packed, jnp.where(row < col, -packed_t, 0.0))
    full = jnp.concatenate(
        [jnp.concatenate([re, -im], axis=1), jnp.concatenate([im, re], axis=1)], axis=0
    )
    high = full.astype(BF16)
    rest = (full - high.astype(F32)).astype(BF16)
    sums = jnp.sum(local_ref[...], axis=0)
    inverse = 1.0 / sums[PIECE - 1 : PIECE, :]
    sums = sums * inverse
    pieces = out_ref.shape[0]
    for d in range(pieces):
        out_ref[d] = sums
    slabs = high_ref.shape[0]
    for s in range(0, slabs, 2):
        cols = jnp.concatenate([high_ref[s], high_ref[s + 1]], axis=1)
        prod = mm(high, cols) + mm(rest, cols)
        for t in range(2):
            rho = jnp.sum(
                other_ref[s + t] * prod[:, LANES * t : LANES * (t + 1)], axis=0, keepdims=True
            )
            out_ref[owner_ref[s + t], PIECE - 1 : PIECE, :] = rho * inverse


def unpack_kernel(pole_total, orbital_count):
    n = orbital_count

    def kernel(in_ref, green_ref, charge_ref, flat_ref):
        per = PIECE - 1
        total = None
        for d in range(in_ref.shape[0]):
            flat_ref[per * d : per * (d + 1), :] = in_ref[d, 0:per, :]
            own = in_ref[d, per:PIECE, :]
            total = own if total is None else total + own
        charge_ref[...] = total
        for q in range(pole_total):
            g, j = divmod(q, WIDE)
            for c in range(2):
                base = n * (2 * g + c)
                green_ref[q, c] = flat_ref[base : base + n, n * j : n * (j + 1)]

    return kernel


def whole(memory=None):
    return pl.BlockSpec(memory_space=memory or pltpu.VMEM)


def local(energy, projector, self_energy, multiplicity, orbitals, owner, rotation):
    pole_total = self_energy.shape[0]
    n = self_energy.shape[2]
    slabs = orbitals.shape[3]
    peers = lax.axis_size("ka")
    poles = lax.axis_size("freq")
    bands = projector.shape[2]
    thermal_level = 0.25 / (pole_total * poles)
    groups = -(-pole_total // WIDE)
    flat_rows = 2 * n * groups
    assert flat_rows == (PIECE - 1) * peers and bands == LANES

    dens, rows = pl.pallas_call(
        green_kernel(pole_total, n, poles, thermal_level),
        out_shape=(
            jax.ShapeDtypeStruct((bands, bands), F32),
            jax.ShapeDtypeStruct((peers, PIECE, LANES), F32),
        ),
        in_specs=[whole(pltpu.SMEM), whole(), whole(), whole(), whole()],
        out_specs=(whole(), whole()),
        scratch_shapes=[pltpu.VMEM((flat_rows, LANES), F32)],
        name="green",
    )(multiplicity, energy, jnp.swapaxes(projector, 2, 3), self_energy, rotation)

    rows_in = lax.all_to_all(rows, "ka", 0, 0, tiled=True)
    dens_in = lax.all_to_all(
        jnp.broadcast_to(dens[None], (poles, *dens.shape)), "freq", 0, 0, tiled=True
    )

    step = 8
    high, other = pl.pallas_call(
        split_kernel,
        grid=(slabs // step,),
        in_specs=[pl.BlockSpec((1, 2, bands, step, LANES), lambda i: (0, 0, 0, i, 0))],
        out_specs=(
            pl.BlockSpec((step, 2 * bands, LANES), lambda i: (i, 0, 0)),
            pl.BlockSpec((step, 2 * bands, LANES), lambda i: (i, 0, 0)),
        ),
        out_shape=(
            jax.ShapeDtypeStruct((slabs, 2 * bands, LANES), BF16),
            jax.ShapeDtypeStruct((slabs, 2 * bands, LANES), F32),
        ),
        name="split",
    )(orbitals)

    sends = pl.pallas_call(
        charge_kernel,
        out_shape=jax.ShapeDtypeStruct((peers, PIECE, LANES), F32),
        in_specs=[whole(pltpu.SMEM), whole(), whole(), whole(), whole()],
        out_specs=whole(),
        name="charge",
    )(owner, dens_in, rows_in, high, other)
    back = lax.all_to_all(sends, "ka", 0, 0, tiled=True)

    local_green, slab = pl.pallas_call(
        unpack_kernel(pole_total, n),
        out_shape=(
            jax.ShapeDtypeStruct((pole_total, 2, n, n), F32),
            jax.ShapeDtypeStruct((1, LANES), F32),
        ),
        in_specs=[whole()],
        out_specs=(whole(), whole()),
        scratch_shapes=[pltpu.VMEM((flat_rows, LANES), F32)],
        name="unpack",
    )(back)
    return (local_green, slab)


def solution(mesh):
    in_specs = (
        P("ka", None),
        P("ka", None, None, None),
        P("freq", None, None, None),
        P("ka"),
        P("ka", None, None, None, "freq"),
        P(),
        P(),
    )
    out_specs = (P("freq", None, None, None), P("ka", "freq"))
    return jax.shard_map(local, mesh=mesh, in_specs=in_specs, out_specs=out_specs, check_vma=False)
```

```python
import math

import jax
import jax.numpy as jnp
from jax import lax
from jax.experimental import pallas as pl
from jax.experimental.pallas import tpu as pltpu
from jax.sharding import PartitionSpec as P


F32 = jnp.float32
BF16 = jnp.bfloat16
LANES = 128
WIDE = 3
PIECE = 16


def low(x):
    return x - x.astype(BF16).astype(F32)


def mm(a, b):
    return jnp.dot(a, b, preferred_element_type=F32)


def mm3(a, b, b_low):
    rows = a.shape[0]
    both = mm(jnp.concatenate([a, low(a)], axis=0), b)
    return both[:rows] + both[rows:] + mm(a, b_low)


def blocks(wide, masks):
    n = wide.shape[0]
    rows = [jnp.where(m, wide, 0.0) for m in masks]
    rows.append(jnp.zeros((LANES - WIDE * n, LANES), F32))
    return jnp.concatenate(rows, axis=0)


def block_weights(wide, masks):
    def form(w):
        re = blocks(w[:, :LANES], masks)
        im = blocks(w[:, LANES:], masks)
        return jnp.concatenate(
            [jnp.concatenate([re, im], axis=1), jnp.concatenate([-im, re], axis=1)], axis=0
        )

    return form(wide), form(low(wide))


def green_kernel(pole_total, orbital_count, pole_stride, thermal_level):
    groups = -(-pole_total // WIDE)
    n = orbital_count

    def kernel(
        mult_ref, energy_ref, proj_ref, self_hbm, rot_ref, dens_ref, rows_ref, flat_ref, self_ref, sem
    ):
        fetch = pltpu.make_async_copy(self_hbm, self_ref, sem)
        fetch.start()
        weight = mult_ref[0].astype(F32)
        shift = lax.axis_index("freq")
        lane = lax.broadcasted_iota(jnp.int32, (n, LANES), 1)
        masks = [(lane >= n * j) & (lane < n * (j + 1)) for j in range(WIDE)]
        energy = energy_ref[...]
        pt = (proj_ref[0, 0], proj_ref[0, 1])
        step = math.pi * thermal_level

        def spread(x):
            tail = jnp.zeros((LANES - WIDE * n, LANES), F32)
            return jnp.concatenate([x] * WIDE + [tail], axis=0).T

        p3 = (spread(pt[0]), spread(pt[1]))
        energy_col = jnp.broadcast_to(energy, (LANES, LANES)).T
        rot = rot_ref[...]
        pt_both = jnp.concatenate([pt[0], pt[1]], axis=1)
        rot_t = rot.T
        turned = mm3(rot_t, pt_both, low(pt_both))
        left = jnp.concatenate([pt_both, turned], axis=0)
        rot_wide = jnp.concatenate([rot] * WIDE + [jnp.zeros((n, LANES - WIDE * n), F32)], axis=1)
        zero = jnp.zeros((LANES, LANES), F32)

        def rot_form(w):
            b = blocks(w, masks)
            return jnp.concatenate(
                [jnp.concatenate([b, zero], axis=1), jnp.concatenate([zero, b], axis=1)], axis=0
            )

        lane_row = lax.broadcasted_iota(jnp.int32, (1, LANES), 1)
        block_of = jnp.where(lane_row >= 2 * n, 2, jnp.where(lane_row >= n, 1, 0))

        gp = []
        for g in range(groups):
            slot = block_of + WIDE * g
            pole = (2 * (slot * pole_stride + shift) + 1).astype(F32) * step
            inv = 1.0 / (pole * pole + energy_col * energy_col)
            br = -energy_col * inv
            bi = -pole * inv
            gp.append((br * p3[0] - bi * p3[1], br * p3[1] + bi * p3[0]))

        big = []
        for g in range(groups):
            xr, xi = gp[g]

            def form(r, i):
                return jnp.concatenate(
                    [jnp.concatenate([r, i], axis=1), jnp.concatenate([i, -r], axis=1)], axis=0
                )

            big.append(mm3(left, form(xr, xi), form(low(xr), low(xi))))
        stacked = jnp.concatenate(big, axis=0)
        right = mm3(stacked, rot_form(rot_wide), rot_form(low(rot_wide)))
        small_right = [right[2 * n * g : 2 * n * g + n] for g in range(groups)]
        both_right = [right[2 * n * g + n : 2 * n * (g + 1)] for g in range(groups)]

        fetch.wait()
        sig = []
        pad = jnp.zeros((n, LANES - WIDE * n), F32)
        none = jnp.zeros((n, n), F32)
        for g in range(groups):
            halves = []
            for c in range(2):
                parts = []
                for j in range(WIDE):
                    q = WIDE * g + j
                    parts.append(self_ref[q, c] if q < pole_total else none)
                halves.append(jnp.concatenate(parts + [pad], axis=1))
            sig.append(jnp.concatenate(halves, axis=1))

        first = [mm3(big[g], *block_weights(sig[g], masks)) for g in range(groups)]
        a1 = [f[:n] for f in first]
        a1_left = [f[n:] for f in first]
        a2 = [mm3(a1[g], *block_weights(a1[g], masks)) for g in range(groups)]
        total = []
        for g in range(groups):
            w = block_weights(a2[g], masks)
            a34 = mm3(jnp.concatenate([a1[g], a2[g]], axis=0), *w)
            a34 = a34[:n] + a34[n:]
            total.append(a1[g] + a2[g] + a34 + mm3(a34, *w))
        last = [
            mm3(jnp.concatenate([sig[g], a1_left[g]], axis=0), *block_weights(total[g], masks))
            for g in range(groups)
        ]
        dress = [sig[g] + last[g][:n] for g in range(groups)]

        acc = None
        for g in range(groups):
            xr, xi = gp[g]
            w = mm3(jnp.concatenate([xr, xi], axis=1), *block_weights(dress[g], masks))
            res, ims = [], []
            for j in range(WIDE):
                q = WIDE * g + j
                pole = (2 * (q * pole_stride + shift) + 1).astype(F32) * step
                inv = 1.0 / (pole * pole + energy * energy)
                br = -energy * inv
                bi = -pole * inv
                res.append(pt[0] * br + pt[1] * bi)
                ims.append(pt[0] * bi - pt[1] * br)
            tail = jnp.zeros((LANES - WIDE * n, LANES), F32)
            re = jnp.concatenate(res + [tail], axis=0)
            im = jnp.concatenate(ims + [tail], axis=0)

            def form(r, i):
                return jnp.concatenate(
                    [jnp.concatenate([r, i], axis=1), jnp.concatenate([-i, r], axis=1)], axis=0
                )

            part = mm3(w, form(re, im), form(low(re), low(im)))
            acc = part if acc is None else acc + part
        er = acc[:, :LANES]
        ei = acc[:, LANES:]
        row = lax.broadcasted_iota(jnp.int32, (LANES, LANES), 0)
        col = lax.broadcasted_iota(jnp.int32, (LANES, LANES), 1)
        scale = weight * thermal_level
        dens_ref[...] = scale * jnp.where(row <= col, er + er.T, ei - ei.T)

        for g in range(groups):
            out = both_right[g] + mm3(
                a1_left[g] + last[g][n:], *block_weights(small_right[g], masks)
            )
            out = weight * out
            flat_ref[2 * n * g : 2 * n * g + n, :] = out[:, :LANES]
            flat_ref[2 * n * g + n : 2 * n * (g + 1), :] = out[:, LANES:]
        per = PIECE - 1
        for d in range(rows_ref.shape[0]):
            rows_ref[d, 0:per, :] = flat_ref[per * d : per * (d + 1), :]
            rows_ref[d, per:PIECE, :] = jnp.broadcast_to(weight, (1, LANES))

    return kernel


def split_kernel(orb_ref, high_ref, other_ref):
    bands = 2 * orb_ref.shape[2]
    slabs = orb_ref.shape[3]
    flat = orb_ref.reshape(bands * slabs, LANES)
    base = pl.program_id(0) * slabs
    for s in range(slabs):
        x = flat[pl.ds(s, bands, stride=slabs), :]
        h = x.astype(BF16)
        high_ref[base + s] = h
        other_ref[base + s] = 2.0 * x - h.astype(F32)


def slab_kernel(mine_ref, theirs_ref, high_ref, other_ref, out_ref):
    packed = mine_ref[...] + theirs_ref[...]
    packed_t = packed.T
    row = lax.broadcasted_iota(jnp.int32, packed.shape, 0)
    col = lax.broadcasted_iota(jnp.int32, packed.shape, 1)
    re = jnp.where(row <= col, packed, packed_t)
    im = jnp.where(row > col, packed, jnp.where(row < col, -packed_t, 0.0))
    full = jnp.concatenate(
        [jnp.concatenate([re, -im], axis=1), jnp.concatenate([im, re], axis=1)], axis=0
    )
    high = full.astype(BF16)
    rest = (full - high.astype(F32)).astype(BF16)
    slabs = high_ref.shape[0]
    for s in range(0, slabs, 2):
        cols = jnp.concatenate([high_ref[s], high_ref[s + 1]], axis=1)
        prod = mm(high, cols) + mm(rest, cols)
        for t in range(2):
            rho = jnp.sum(
                other_ref[s + t] * prod[:, LANES * t : LANES * (t + 1)], axis=0, keepdims=True
            )
            out_ref[s + t : s + t + 1, :] = rho


def pack_kernel(owner_ref, local_ref, charge_ref, out_ref):
    sums = jnp.sum(local_ref[...], axis=0)
    inverse = 1.0 / sums[PIECE - 1 : PIECE, :]
    sums = sums * inverse
    for d in range(out_ref.shape[0]):
        out_ref[d] = sums
    for s in range(charge_ref.shape[0]):
        out_ref[owner_ref[s], PIECE - 1 : PIECE, :] = charge_ref[s : s + 1, :] * inverse


def unpack_kernel(pole_total, orbital_count):
    n = orbital_count

    def kernel(in_ref, green_ref, charge_ref, flat_ref):
        per = PIECE - 1
        total = None
        for d in range(in_ref.shape[0]):
            flat_ref[per * d : per * (d + 1), :] = in_ref[d, 0:per, :]
            own = in_ref[d, per:PIECE, :]
            total = own if total is None else total + own
        charge_ref[...] = total
        for q in range(pole_total):
            g, j = divmod(q, WIDE)
            for c in range(2):
                base = n * (2 * g + c)
                green_ref[q, c] = flat_ref[base : base + n, n * j : n * (j + 1)]

    return kernel


def whole(memory=None):
    return pl.BlockSpec(memory_space=memory or pltpu.VMEM)


def held(x):
    return pltpu.with_memory_space_constraint(x, pltpu.VMEM)


def far(x):
    return pltpu.with_memory_space_constraint(x, pltpu.HBM)


def local(energy, projector, self_energy, multiplicity, orbitals, owner, rotation):
    pole_total = self_energy.shape[0]
    n = self_energy.shape[2]
    slabs = orbitals.shape[3]
    peers = lax.axis_size("ka")
    poles = lax.axis_size("freq")
    bands = projector.shape[2]
    thermal_level = 0.25 / (pole_total * poles)
    groups = -(-pole_total // WIDE)
    flat_rows = 2 * n * groups
    assert flat_rows == (PIECE - 1) * peers and bands == LANES

    dens, rows = pl.pallas_call(
        green_kernel(pole_total, n, poles, thermal_level),
        out_shape=(
            pltpu.VMEM((bands, bands), F32),
            pltpu.VMEM((peers, PIECE, LANES), F32),
        ),
        in_specs=[whole(pltpu.SMEM), whole(), whole(), whole(pl.ANY), whole()],
        out_specs=(whole(), whole()),
        scratch_shapes=[
            pltpu.VMEM((flat_rows, LANES), F32),
            pltpu.VMEM(self_energy.shape, F32),
            pltpu.SemaphoreType.DMA,
        ],
        compiler_params=pltpu.CompilerParams(vmem_limit_bytes=20 << 20),
        name="green",
    )(
        multiplicity,
        far(energy),
        far(jnp.swapaxes(projector, 2, 3)),
        far(self_energy),
        far(rotation),
    )

    def swapped(x, flip):
        return lax.ppermute(x, "freq", [(i, i ^ flip) for i in range(poles)])

    theirs = swapped(dens, 4)
    rows_in = lax.all_to_all(rows, "ka", 0, 0, tiled=True)
    dens = dens + theirs
    dens = dens + swapped(dens, 1)
    theirs = swapped(dens, 3)

    step = 8
    high, other = pl.pallas_call(
        split_kernel,
        grid=(slabs // step,),
        in_specs=[pl.BlockSpec((1, 2, bands, step, LANES), lambda i: (0, 0, 0, i, 0))],
        out_specs=(whole(), whole()),
        out_shape=(
            pltpu.VMEM((slabs, 2 * bands, LANES), BF16),
            pltpu.VMEM((slabs, 2 * bands, LANES), F32),
        ),
        compiler_params=pltpu.CompilerParams(vmem_limit_bytes=8 << 20),
        name="split",
    )(far(orbitals))

    rho = pl.pallas_call(
        slab_kernel,
        out_shape=pltpu.VMEM((slabs, LANES), F32),
        in_specs=[whole()] * 4,
        out_specs=whole(),
        compiler_params=pltpu.CompilerParams(vmem_limit_bytes=8 << 20),
        name="slab",
    )(held(dens), held(theirs), held(high), held(other))
    sends = pl.pallas_call(
        pack_kernel,
        out_shape=pltpu.VMEM((peers, PIECE, LANES), F32),
        in_specs=[whole(pltpu.SMEM), whole(), whole()],
        out_specs=whole(),
        compiler_params=pltpu.CompilerParams(vmem_limit_bytes=4 << 20),
        name="pack",
    )(owner, held(rows_in), held(rho))
    back = lax.all_to_all(sends, "ka", 0, 0, tiled=True)

    local_green, slab = pl.pallas_call(
        unpack_kernel(pole_total, n),
        out_shape=(
            jax.ShapeDtypeStruct((pole_total, 2, n, n), F32),
            jax.ShapeDtypeStruct((1, LANES), F32),
        ),
        in_specs=[whole()],
        out_specs=(whole(), whole()),
        scratch_shapes=[pltpu.VMEM((flat_rows, LANES), F32)],
        compiler_params=pltpu.CompilerParams(vmem_limit_bytes=6 << 20),
        name="unpack",
    )(held(back))
    return (local_green, slab)


def solution(mesh):
    in_specs = (
        P("ka", None),
        P("ka", None, None, None),
        P("freq", None, None, None),
        P("ka"),
        P("ka", None, None, None, "freq"),
        P(),
        P(),
    )
    out_specs = (P("freq", None, None, None), P("ka", "freq"))
    return jax.shard_map(local, mesh=mesh, in_specs=in_specs, out_specs=out_specs, check_vma=False)
```

```python
import math

import jax
import jax.numpy as jnp
from jax import lax
from jax.experimental import pallas as pl
from jax.experimental.pallas import tpu as pltpu
from jax.sharding import PartitionSpec as P


F32 = jnp.float32
BF16 = jnp.bfloat16
LANES = 128
WIDE = 3
PIECE = 16


def low(x):
    return x - x.astype(BF16).astype(F32)


def mm(a, b):
    return jnp.dot(a, b, preferred_element_type=F32)


def mm3(a, b, b_low):
    rows = a.shape[0]
    both = mm(jnp.concatenate([a, low(a)], axis=0), b)
    return both[:rows] + both[rows:] + mm(a, b_low)


def blocks(wide, masks):
    n = wide.shape[0]
    rows = [jnp.where(m, wide, 0.0) for m in masks]
    rows.append(jnp.zeros((LANES - WIDE * n, LANES), F32))
    return jnp.concatenate(rows, axis=0)


def block_weights(wide, masks):
    def form(w):
        re = blocks(w[:, :LANES], masks)
        im = blocks(w[:, LANES:], masks)
        return jnp.concatenate(
            [jnp.concatenate([re, im], axis=1), jnp.concatenate([-im, re], axis=1)], axis=0
        )

    return form(wide), form(low(wide))


def green_kernel(pole_total, orbital_count, pole_stride, thermal_level):
    groups = -(-pole_total // WIDE)
    n = orbital_count

    def kernel(
        mult_ref,
        energy_ref,
        proj_ref,
        self_hbm,
        rot_ref,
        dens_ref,
        keep_ref,
        give_ref,
        flat_ref,
        rows_ref,
        self_ref,
        sem,
    ):
        fetch = pltpu.make_async_copy(self_hbm, self_ref, sem)
        fetch.start()
        weight = mult_ref[0].astype(F32)
        shift = lax.axis_index("freq")
        lane = lax.broadcasted_iota(jnp.int32, (n, LANES), 1)
        masks = [(lane >= n * j) & (lane < n * (j + 1)) for j in range(WIDE)]
        energy = energy_ref[...]
        pt = (proj_ref[0, 0], proj_ref[0, 1])
        step = math.pi * thermal_level

        def spread(x):
            tail = jnp.zeros((LANES - WIDE * n, LANES), F32)
            return jnp.concatenate([x] * WIDE + [tail], axis=0).T

        p3 = (spread(pt[0]), spread(pt[1]))
        energy_col = jnp.broadcast_to(energy, (LANES, LANES)).T
        rot = rot_ref[...]
        pt_both = jnp.concatenate([pt[0], pt[1]], axis=1)
        rot_t = rot.T
        turned = mm3(rot_t, pt_both, low(pt_both))
        left = jnp.concatenate([pt_both, turned], axis=0)
        rot_wide = jnp.concatenate([rot] * WIDE + [jnp.zeros((n, LANES - WIDE * n), F32)], axis=1)
        zero = jnp.zeros((LANES, LANES), F32)

        def rot_form(w):
            b = blocks(w, masks)
            return jnp.concatenate(
                [jnp.concatenate([b, zero], axis=1), jnp.concatenate([zero, b], axis=1)], axis=0
            )

        lane_row = lax.broadcasted_iota(jnp.int32, (1, LANES), 1)
        block_of = jnp.where(lane_row >= 2 * n, 2, jnp.where(lane_row >= n, 1, 0))

        gp = []
        for g in range(groups):
            slot = block_of + WIDE * g
            pole = (2 * (slot * pole_stride + shift) + 1).astype(F32) * step
            inv = 1.0 / (pole * pole + energy_col * energy_col)
            br = -energy_col * inv
            bi = -pole * inv
            gp.append((br * p3[0] - bi * p3[1], br * p3[1] + bi * p3[0]))

        big = []
        for g in range(groups):
            xr, xi = gp[g]

            def form(r, i):
                return jnp.concatenate(
                    [jnp.concatenate([r, i], axis=1), jnp.concatenate([i, -r], axis=1)], axis=0
                )

            big.append(mm3(left, form(xr, xi), form(low(xr), low(xi))))
        stacked = jnp.concatenate(big, axis=0)
        right = mm3(stacked, rot_form(rot_wide), rot_form(low(rot_wide)))
        small_right = [right[2 * n * g : 2 * n * g + n] for g in range(groups)]
        both_right = [right[2 * n * g + n : 2 * n * (g + 1)] for g in range(groups)]

        fetch.wait()
        sig = []
        pad = jnp.zeros((n, LANES - WIDE * n), F32)
        none = jnp.zeros((n, n), F32)
        for g in range(groups):
            halves = []
            for c in range(2):
                parts = []
                for j in range(WIDE):
                    q = WIDE * g + j
                    parts.append(self_ref[q, c] if q < pole_total else none)
                halves.append(jnp.concatenate(parts + [pad], axis=1))
            sig.append(jnp.concatenate(halves, axis=1))

        first = [mm3(big[g], *block_weights(sig[g], masks)) for g in range(groups)]
        a1 = [f[:n] for f in first]
        a1_left = [f[n:] for f in first]
        a2 = [mm3(a1[g], *block_weights(a1[g], masks)) for g in range(groups)]
        total = []
        for g in range(groups):
            w = block_weights(a2[g], masks)
            a34 = mm3(jnp.concatenate([a1[g], a2[g]], axis=0), *w)
            a34 = a34[:n] + a34[n:]
            total.append(a1[g] + a2[g] + a34 + mm3(a34, *w))
        last = [
            mm3(jnp.concatenate([sig[g], a1_left[g]], axis=0), *block_weights(total[g], masks))
            for g in range(groups)
        ]
        dress = [sig[g] + last[g][:n] for g in range(groups)]

        acc = None
        for g in range(groups):
            xr, xi = gp[g]
            w = mm3(jnp.concatenate([xr, xi], axis=1), *block_weights(dress[g], masks))
            res, ims = [], []
            for j in range(WIDE):
                q = WIDE * g + j
                pole = (2 * (q * pole_stride + shift) + 1).astype(F32) * step
                inv = 1.0 / (pole * pole + energy * energy)
                br = -energy * inv
                bi = -pole * inv
                res.append(pt[0] * br + pt[1] * bi)
                ims.append(pt[0] * bi - pt[1] * br)
            tail = jnp.zeros((LANES - WIDE * n, LANES), F32)
            re = jnp.concatenate(res + [tail], axis=0)
            im = jnp.concatenate(ims + [tail], axis=0)

            def form(r, i):
                return jnp.concatenate(
                    [jnp.concatenate([r, i], axis=1), jnp.concatenate([-i, r], axis=1)], axis=0
                )

            part = mm3(w, form(re, im), form(low(re), low(im)))
            acc = part if acc is None else acc + part
        er = acc[:, :LANES]
        ei = acc[:, LANES:]
        row = lax.broadcasted_iota(jnp.int32, (LANES, LANES), 0)
        col = lax.broadcasted_iota(jnp.int32, (LANES, LANES), 1)
        scale = weight * thermal_level
        dens_ref[...] = scale * jnp.where(row <= col, er + er.T, ei - ei.T)

        for g in range(groups):
            out = both_right[g] + mm3(
                a1_left[g] + last[g][n:], *block_weights(small_right[g], masks)
            )
            out = weight * out
            flat_ref[2 * n * g : 2 * n * g + n, :] = out[:, :LANES]
            flat_ref[2 * n * g + n : 2 * n * (g + 1), :] = out[:, LANES:]
        per = PIECE - 1
        for d in range(rows_ref.shape[0]):
            rows_ref[d, 0:per, :] = flat_ref[per * d : per * (d + 1), :]
            rows_ref[d, per:PIECE, :] = jnp.broadcast_to(weight, (1, LANES))
        me = lax.axis_index("ka")
        half = keep_ref.shape[0]
        for r in range(half):
            d = ((r % 4) * 8 + (r // 4) * 2) ^ me
            keep_ref[r] = rows_ref[d]
            give_ref[r] = rows_ref[d ^ 1]

    return kernel


def split_kernel(orb_ref, high_ref, other_ref):
    bands = 2 * orb_ref.shape[2]
    slabs = orb_ref.shape[3]
    flat = orb_ref.reshape(bands * slabs, LANES)
    base = pl.program_id(0) * slabs
    for s in range(slabs):
        x = flat[pl.ds(s, bands, stride=slabs), :]
        h = x.astype(BF16)
        high_ref[base + s] = h
        other_ref[base + s] = 2.0 * x - h.astype(F32)


def slab_kernel(mine_ref, theirs_ref, high_ref, other_ref, out_ref):
    packed = mine_ref[...] + theirs_ref[...]
    packed_t = packed.T
    row = lax.broadcasted_iota(jnp.int32, packed.shape, 0)
    col = lax.broadcasted_iota(jnp.int32, packed.shape, 1)
    re = jnp.where(row <= col, packed, packed_t)
    im = jnp.where(row > col, packed, jnp.where(row < col, -packed_t, 0.0))
    full = jnp.concatenate(
        [jnp.concatenate([re, -im], axis=1), jnp.concatenate([im, re], axis=1)], axis=0
    )
    high = full.astype(BF16)
    rest = (full - high.astype(F32)).astype(BF16)
    slabs = high_ref.shape[0]
    for s in range(0, slabs, 2):
        cols = jnp.concatenate([high_ref[s], high_ref[s + 1]], axis=1)
        prod = mm(high, cols) + mm(rest, cols)
        for t in range(2):
            rho = jnp.sum(
                other_ref[s + t] * prod[:, LANES * t : LANES * (t + 1)], axis=0, keepdims=True
            )
            out_ref[s + t : s + t + 1, :] = rho


def pack_kernel(owner_ref, a_ref, b_ref, c_ref, d_ref, charge_ref, out_ref):
    sums = (a_ref[...] + b_ref[...]) + (c_ref[...] + d_ref[...])
    inverse = 1.0 / sums[PIECE - 1 : PIECE, :]
    sums = sums * inverse
    for d in range(out_ref.shape[0]):
        out_ref[d] = sums
    for s in range(charge_ref.shape[0]):
        out_ref[owner_ref[s], PIECE - 1 : PIECE, :] = charge_ref[s : s + 1, :] * inverse


def unpack_kernel(pole_total, orbital_count):
    n = orbital_count

    def kernel(in_ref, green_ref, charge_ref, flat_ref):
        per = PIECE - 1
        total = None
        for d in range(in_ref.shape[0]):
            flat_ref[per * d : per * (d + 1), :] = in_ref[d, 0:per, :]
            own = in_ref[d, per:PIECE, :]
            total = own if total is None else total + own
        charge_ref[...] = total
        for q in range(pole_total):
            g, j = divmod(q, WIDE)
            for c in range(2):
                base = n * (2 * g + c)
                green_ref[q, c] = flat_ref[base : base + n, n * j : n * (j + 1)]

    return kernel


def whole(memory=None):
    return pl.BlockSpec(memory_space=memory or pltpu.VMEM)


def held(x):
    return pltpu.with_memory_space_constraint(x, pltpu.VMEM)


def far(x):
    return pltpu.with_memory_space_constraint(x, pltpu.HBM)


def local(energy, projector, self_energy, multiplicity, orbitals, owner, rotation):
    pole_total = self_energy.shape[0]
    n = self_energy.shape[2]
    slabs = orbitals.shape[3]
    peers = lax.axis_size("ka")
    poles = lax.axis_size("freq")
    bands = projector.shape[2]
    thermal_level = 0.25 / (pole_total * poles)
    groups = -(-pole_total // WIDE)
    flat_rows = 2 * n * groups
    assert flat_rows == (PIECE - 1) * peers and bands == LANES

    dens, keep, give = pl.pallas_call(
        green_kernel(pole_total, n, poles, thermal_level),
        out_shape=(
            pltpu.VMEM((bands, bands), F32),
            pltpu.VMEM((peers // 2, PIECE, LANES), F32),
            pltpu.VMEM((peers // 2, PIECE, LANES), F32),
        ),
        in_specs=[whole(pltpu.SMEM), whole(), whole(), whole(pl.ANY), whole()],
        out_specs=(whole(), whole(), whole()),
        scratch_shapes=[
            pltpu.VMEM((flat_rows, LANES), F32),
            pltpu.VMEM((peers, PIECE, LANES), F32),
            pltpu.VMEM(self_energy.shape, F32),
            pltpu.SemaphoreType.DMA,
        ],
        compiler_params=pltpu.CompilerParams(vmem_limit_bytes=20 << 20),
        name="green",
    )(
        multiplicity,
        far(energy),
        far(jnp.swapaxes(projector, 2, 3)),
        far(self_energy),
        far(rotation),
    )

    def swapped(x, axis, flip):
        return lax.ppermute(x, axis, [(i, i ^ flip) for i in range(lax.axis_size(axis))])

    theirs = swapped(give, "ka", 1)
    other_dens = swapped(dens, "freq", 4)
    rows = (keep + theirs).reshape(4, 4, PIECE, LANES)
    arrived = [swapped(rows[d], "ka", 2 * d) for d in range(1, 4)]
    rows = rows[0] + sum(arrived)
    dens = dens + other_dens
    other_dens = swapped(dens, "freq", 1)
    dens = dens + other_dens
    parts = [rows[0]] + [swapped(rows[d], "ka", 8 * d) for d in range(1, 4)]
    theirs = swapped(dens, "freq", 3)

    step = 8
    high, other = pl.pallas_call(
        split_kernel,
        grid=(slabs // step,),
        in_specs=[pl.BlockSpec((1, 2, bands, step, LANES), lambda i: (0, 0, 0, i, 0))],
        out_specs=(whole(), whole()),
        out_shape=(
            pltpu.VMEM((slabs, 2 * bands, LANES), BF16),
            pltpu.VMEM((slabs, 2 * bands, LANES), F32),
        ),
        compiler_params=pltpu.CompilerParams(vmem_limit_bytes=8 << 20),
        name="split",
    )(far(orbitals))
    rho = pl.pallas_call(
        slab_kernel,
        out_shape=pltpu.VMEM((slabs, LANES), F32),
        in_specs=[whole()] * 4,
        out_specs=whole(),
        compiler_params=pltpu.CompilerParams(vmem_limit_bytes=8 << 20),
        name="slab",
    )(held(dens), held(theirs), held(high), held(other))
    sends = pl.pallas_call(
        pack_kernel,
        out_shape=pltpu.VMEM((peers, PIECE, LANES), F32),
        in_specs=[whole(pltpu.SMEM)] + [whole()] * 5,
        out_specs=whole(),
        compiler_params=pltpu.CompilerParams(vmem_limit_bytes=4 << 20),
        name="pack",
    )(owner, *[held(x) for x in parts], held(rho))
    back = lax.all_to_all(sends, "ka", 0, 0, tiled=True)

    local_green, slab = pl.pallas_call(
        unpack_kernel(pole_total, n),
        out_shape=(
            jax.ShapeDtypeStruct((pole_total, 2, n, n), F32),
            jax.ShapeDtypeStruct((1, LANES), F32),
        ),
        in_specs=[whole()],
        out_specs=(whole(), whole()),
        scratch_shapes=[pltpu.VMEM((flat_rows, LANES), F32)],
        compiler_params=pltpu.CompilerParams(vmem_limit_bytes=6 << 20),
        name="unpack",
    )(held(back))
    return (local_green, slab)


def solution(mesh):
    in_specs = (
        P("ka", None),
        P("ka", None, None, None),
        P("freq", None, None, None),
        P("ka"),
        P("ka", None, None, None, "freq"),
        P(),
        P(),
    )
    out_specs = (P("freq", None, None, None), P("ka", "freq"))
    return jax.shard_map(local, mesh=mesh, in_specs=in_specs, out_specs=out_specs, check_vma=False)
```

```python
import math

import jax
import jax.numpy as jnp
from jax import lax
from jax.experimental import pallas as pl
from jax.experimental.pallas import tpu as pltpu
from jax.sharding import PartitionSpec as P


F32 = jnp.float32
BF16 = jnp.bfloat16
LANES = 128
WIDE = 3
PIECE = 16


def low(x):
    return x - x.astype(BF16).astype(F32)


def mm(a, b):
    return jnp.dot(a, b, preferred_element_type=F32)


def mm3(a, b, b_low):
    rows = a.shape[0]
    both = mm(jnp.concatenate([a, low(a)], axis=0), b)
    return both[:rows] + both[rows:] + mm(a, b_low)


def blocks(wide, masks):
    n = wide.shape[0]
    rows = [jnp.where(m, wide, 0.0) for m in masks]
    rows.append(jnp.zeros((LANES - WIDE * n, LANES), F32))
    return jnp.concatenate(rows, axis=0)


def block_weights(wide, masks):
    def form(w):
        re = blocks(w[:, :LANES], masks)
        im = blocks(w[:, LANES:], masks)
        return jnp.concatenate(
            [jnp.concatenate([re, im], axis=1), jnp.concatenate([-im, re], axis=1)], axis=0
        )

    return form(wide), form(low(wide))


def green_kernel(pole_total, orbital_count, pole_stride, thermal_level):
    groups = -(-pole_total // WIDE)
    n = orbital_count

    def kernel(
        mult_ref, energy_ref, proj_ref, self_hbm, rot_ref, dens_ref, rows_ref, flat_ref, self_ref, sem
    ):
        fetch = pltpu.make_async_copy(self_hbm, self_ref, sem)
        fetch.start()
        weight = mult_ref[0].astype(F32)
        shift = lax.axis_index("freq")
        lane = lax.broadcasted_iota(jnp.int32, (n, LANES), 1)
        masks = [(lane >= n * j) & (lane < n * (j + 1)) for j in range(WIDE)]
        energy = energy_ref[...]
        pt = (proj_ref[0, 0], proj_ref[0, 1])
        step = math.pi * thermal_level

        def spread(x):
            tail = jnp.zeros((LANES - WIDE * n, LANES), F32)
            return jnp.concatenate([x] * WIDE + [tail], axis=0).T

        p3 = (spread(pt[0]), spread(pt[1]))
        energy_col = jnp.broadcast_to(energy, (LANES, LANES)).T
        rot = rot_ref[...]
        pt_both = jnp.concatenate([pt[0], pt[1]], axis=1)
        rot_t = rot.T
        turned = mm3(rot_t, pt_both, low(pt_both))
        left = jnp.concatenate([pt_both, turned], axis=0)
        rot_wide = jnp.concatenate([rot] * WIDE + [jnp.zeros((n, LANES - WIDE * n), F32)], axis=1)
        zero = jnp.zeros((LANES, LANES), F32)

        def rot_form(w):
            b = blocks(w, masks)
            return jnp.concatenate(
                [jnp.concatenate([b, zero], axis=1), jnp.concatenate([zero, b], axis=1)], axis=0
            )

        lane_row = lax.broadcasted_iota(jnp.int32, (1, LANES), 1)
        block_of = jnp.where(lane_row >= 2 * n, 2, jnp.where(lane_row >= n, 1, 0))

        gp = []
        for g in range(groups):
            slot = block_of + WIDE * g
            pole = (2 * (slot * pole_stride + shift) + 1).astype(F32) * step
            inv = 1.0 / (pole * pole + energy_col * energy_col)
            br = -energy_col * inv
            bi = -pole * inv
            gp.append((br * p3[0] - bi * p3[1], br * p3[1] + bi * p3[0]))

        big = []
        for g in range(groups):
            xr, xi = gp[g]

            def form(r, i):
                return jnp.concatenate(
                    [jnp.concatenate([r, i], axis=1), jnp.concatenate([i, -r], axis=1)], axis=0
                )

            big.append(mm3(left, form(xr, xi), form(low(xr), low(xi))))
        stacked = jnp.concatenate(big, axis=0)
        right = mm3(stacked, rot_form(rot_wide), rot_form(low(rot_wide)))
        small_right = [right[2 * n * g : 2 * n * g + n] for g in range(groups)]
        both_right = [right[2 * n * g + n : 2 * n * (g + 1)] for g in range(groups)]

        fetch.wait()
        sig = []
        pad = jnp.zeros((n, LANES - WIDE * n), F32)
        none = jnp.zeros((n, n), F32)
        for g in range(groups):
            halves = []
            for c in range(2):
                parts = []
                for j in range(WIDE):
                    q = WIDE * g + j
                    parts.append(self_ref[q, c] if q < pole_total else none)
                halves.append(jnp.concatenate(parts + [pad], axis=1))
            sig.append(jnp.concatenate(halves, axis=1))

        first = [mm3(big[g], *block_weights(sig[g], masks)) for g in range(groups)]
        a1 = [f[:n] for f in first]
        a1_left = [f[n:] for f in first]
        a2 = [mm3(a1[g], *block_weights(a1[g], masks)) for g in range(groups)]
        total = []
        for g in range(groups):
            w = block_weights(a2[g], masks)
            a34 = mm3(jnp.concatenate([a1[g], a2[g]], axis=0), *w)
            a34 = a34[:n] + a34[n:]
            total.append(a1[g] + a2[g] + a34 + mm3(a34, *w))
        last = [
            mm3(jnp.concatenate([sig[g], a1_left[g]], axis=0), *block_weights(total[g], masks))
            for g in range(groups)
        ]
        dress = [sig[g] + last[g][:n] for g in range(groups)]

        acc = None
        for g in range(groups):
            xr, xi = gp[g]
            w = mm3(jnp.concatenate([xr, xi], axis=1), *block_weights(dress[g], masks))
            res, ims = [], []
            for j in range(WIDE):
                q = WIDE * g + j
                pole = (2 * (q * pole_stride + shift) + 1).astype(F32) * step
                inv = 1.0 / (pole * pole + energy * energy)
                br = -energy * inv
                bi = -pole * inv
                res.append(pt[0] * br + pt[1] * bi)
                ims.append(pt[0] * bi - pt[1] * br)
            tail = jnp.zeros((LANES - WIDE * n, LANES), F32)
            re = jnp.concatenate(res + [tail], axis=0)
            im = jnp.concatenate(ims + [tail], axis=0)

            def form(r, i):
                return jnp.concatenate(
                    [jnp.concatenate([r, i], axis=1), jnp.concatenate([-i, r], axis=1)], axis=0
                )

            part = mm3(w, form(re, im), form(low(re), low(im)))
            acc = part if acc is None else acc + part
        er = acc[:, :LANES]
        ei = acc[:, LANES:]
        row = lax.broadcasted_iota(jnp.int32, (LANES, LANES), 0)
        col = lax.broadcasted_iota(jnp.int32, (LANES, LANES), 1)
        scale = weight * thermal_level
        dens_ref[...] = scale * jnp.where(row <= col, er + er.T, ei - ei.T)

        for g in range(groups):
            out = both_right[g] + mm3(
                a1_left[g] + last[g][n:], *block_weights(small_right[g], masks)
            )
            out = weight * out
            flat_ref[2 * n * g : 2 * n * g + n, :] = out[:, :LANES]
            flat_ref[2 * n * g + n : 2 * n * (g + 1), :] = out[:, LANES:]
        per = PIECE - 1
        for d in range(rows_ref.shape[0]):
            rows_ref[d, 0:per, :] = flat_ref[per * d : per * (d + 1), :]
            rows_ref[d, per:PIECE, :] = jnp.broadcast_to(weight, (1, LANES))

    return kernel


def split_kernel(orb_ref, high_ref, other_ref):
    bands = 2 * orb_ref.shape[2]
    slabs = orb_ref.shape[3]
    flat = orb_ref.reshape(bands * slabs, LANES)
    base = pl.program_id(0) * slabs
    for s in range(slabs):
        x = flat[pl.ds(s, bands, stride=slabs), :]
        h = x.astype(BF16)
        high_ref[base + s] = h
        other_ref[base + s] = 2.0 * x - h.astype(F32)


def slab_kernel(a_ref, b_ref, c_ref, d_ref, high_ref, other_ref, out_ref):
    packed = (a_ref[...] + b_ref[...]) + (c_ref[...] + d_ref[...])
    packed_t = packed.T
    row = lax.broadcasted_iota(jnp.int32, packed.shape, 0)
    col = lax.broadcasted_iota(jnp.int32, packed.shape, 1)
    re = jnp.where(row <= col, packed, packed_t)
    im = jnp.where(row > col, packed, jnp.where(row < col, -packed_t, 0.0))
    full = jnp.concatenate(
        [jnp.concatenate([re, -im], axis=1), jnp.concatenate([im, re], axis=1)], axis=0
    )
    high = full.astype(BF16)
    rest = (full - high.astype(F32)).astype(BF16)
    slabs = high_ref.shape[0]
    for s in range(0, slabs, 2):
        cols = jnp.concatenate([high_ref[s], high_ref[s + 1]], axis=1)
        prod = mm(high, cols) + mm(rest, cols)
        for t in range(2):
            rho = jnp.sum(
                other_ref[s + t] * prod[:, LANES * t : LANES * (t + 1)], axis=0, keepdims=True
            )
            out_ref[s + t : s + t + 1, :] = rho


def pack_kernel(owner_ref, local_ref, charge_ref, out_ref):
    sums = jnp.sum(local_ref[...], axis=0)
    inverse = 1.0 / sums[PIECE - 1 : PIECE, :]
    sums = sums * inverse
    for d in range(out_ref.shape[0]):
        out_ref[d] = sums
    for s in range(charge_ref.shape[0]):
        out_ref[owner_ref[s], PIECE - 1 : PIECE, :] = charge_ref[s : s + 1, :] * inverse


def unpack_kernel(pole_total, orbital_count):
    n = orbital_count

    def kernel(in_ref, green_ref, charge_ref, flat_ref):
        per = PIECE - 1
        total = None
        for d in range(in_ref.shape[0]):
            flat_ref[per * d : per * (d + 1), :] = in_ref[d, 0:per, :]
            own = in_ref[d, per:PIECE, :]
            total = own if total is None else total + own
        charge_ref[...] = total
        for q in range(pole_total):
            g, j = divmod(q, WIDE)
            for c in range(2):
                base = n * (2 * g + c)
                green_ref[q, c] = flat_ref[base : base + n, n * j : n * (j + 1)]

    return kernel


def whole(memory=None):
    return pl.BlockSpec(memory_space=memory or pltpu.VMEM)


def held(x):
    return pltpu.with_memory_space_constraint(x, pltpu.VMEM)


def far(x):
    return pltpu.with_memory_space_constraint(x, pltpu.HBM)


def local(energy, projector, self_energy, multiplicity, orbitals, owner, rotation):
    pole_total = self_energy.shape[0]
    n = self_energy.shape[2]
    slabs = orbitals.shape[3]
    peers = lax.axis_size("ka")
    poles = lax.axis_size("freq")
    bands = projector.shape[2]
    thermal_level = 0.25 / (pole_total * poles)
    groups = -(-pole_total // WIDE)
    flat_rows = 2 * n * groups
    assert flat_rows == (PIECE - 1) * peers and bands == LANES

    dens, rows = pl.pallas_call(
        green_kernel(pole_total, n, poles, thermal_level),
        out_shape=(
            pltpu.VMEM((bands, bands), F32),
            pltpu.VMEM((peers, PIECE, LANES), F32),
        ),
        in_specs=[whole(pltpu.SMEM), whole(), whole(), whole(pl.ANY), whole()],
        out_specs=(whole(), whole()),
        scratch_shapes=[
            pltpu.VMEM((flat_rows, LANES), F32),
            pltpu.VMEM(self_energy.shape, F32),
            pltpu.SemaphoreType.DMA,
        ],
        compiler_params=pltpu.CompilerParams(vmem_limit_bytes=20 << 20),
        name="green",
    )(
        multiplicity,
        far(energy),
        far(jnp.swapaxes(projector, 2, 3)),
        far(self_energy),
        far(rotation),
    )

    def swapped(x, flip):
        return lax.ppermute(x, "freq", [(i, i ^ flip) for i in range(poles)])

    theirs = swapped(dens, 4)
    rows_in = lax.all_to_all(rows, "ka", 0, 0, tiled=True)
    dens = dens + theirs
    arrived = [swapped(dens, d) for d in range(1, 4)]

    step = 8
    high, other = pl.pallas_call(
        split_kernel,
        grid=(slabs // step,),
        in_specs=[pl.BlockSpec((1, 2, bands, step, LANES), lambda i: (0, 0, 0, i, 0))],
        out_specs=(whole(), whole()),
        out_shape=(
            pltpu.VMEM((slabs, 2 * bands, LANES), BF16),
            pltpu.VMEM((slabs, 2 * bands, LANES), F32),
        ),
        compiler_params=pltpu.CompilerParams(vmem_limit_bytes=8 << 20),
        name="split",
    )(far(orbitals))
    rho = pl.pallas_call(
        slab_kernel,
        out_shape=pltpu.VMEM((slabs, LANES), F32),
        in_specs=[whole()] * 6,
        out_specs=whole(),
        compiler_params=pltpu.CompilerParams(vmem_limit_bytes=8 << 20),
        name="slab",
    )(*[held(x) for x in (dens, *arrived, high, other)])
    sends = pl.pallas_call(
        pack_kernel,
        out_shape=pltpu.VMEM((peers, PIECE, LANES), F32),
        in_specs=[whole(pltpu.SMEM), whole(), whole()],
        out_specs=whole(),
        compiler_params=pltpu.CompilerParams(vmem_limit_bytes=4 << 20),
        name="pack",
    )(owner, held(rows_in), held(rho))
    back = lax.all_to_all(sends, "ka", 0, 0, tiled=True)

    local_green, slab = pl.pallas_call(
        unpack_kernel(pole_total, n),
        out_shape=(
            jax.ShapeDtypeStruct((pole_total, 2, n, n), F32),
            jax.ShapeDtypeStruct((1, LANES), F32),
        ),
        in_specs=[whole()],
        out_specs=(whole(), whole()),
        scratch_shapes=[pltpu.VMEM((flat_rows, LANES), F32)],
        compiler_params=pltpu.CompilerParams(vmem_limit_bytes=6 << 20),
        name="unpack",
    )(held(back))
    return (local_green, slab)


def solution(mesh):
    in_specs = (
        P("ka", None),
        P("ka", None, None, None),
        P("freq", None, None, None),
        P("ka"),
        P("ka", None, None, None, "freq"),
        P(),
        P(),
    )
    out_specs = (P("freq", None, None, None), P("ka", "freq"))
    return jax.shard_map(local, mesh=mesh, in_specs=in_specs, out_specs=out_specs, check_vma=False)
```

```python
import math

import jax
import jax.numpy as jnp
from jax import lax
from jax.experimental import pallas as pl
from jax.experimental.pallas import tpu as pltpu
from jax.sharding import PartitionSpec as P


F32 = jnp.float32
BF16 = jnp.bfloat16
LANES = 128
WIDE = 3
PIECE = 16
USED = 13


def low(x):
    return x - x.astype(BF16).astype(F32)


def mm(a, b):
    return jnp.dot(a, b, preferred_element_type=F32)


def mm3(a, b, b_low):
    rows = a.shape[0]
    both = mm(jnp.concatenate([a, low(a)], axis=0), b)
    return both[:rows] + both[rows:] + mm(a, b_low)


def blocks(wide, masks):
    n = wide.shape[0]
    rows = [jnp.where(m, wide, 0.0) for m in masks]
    rows.append(jnp.zeros((LANES - WIDE * n, LANES), F32))
    return jnp.concatenate(rows, axis=0)


def block_weights(wide, masks):
    def form(w):
        re = blocks(w[:, :LANES], masks)
        im = blocks(w[:, LANES:], masks)
        return jnp.concatenate(
            [jnp.concatenate([re, im], axis=1), jnp.concatenate([-im, re], axis=1)], axis=0
        )

    return form(wide), form(low(wide))


def green_kernel(pole_total, orbital_count, pole_stride, thermal_level):
    groups = -(-pole_total // WIDE)
    n = orbital_count

    def kernel(
        mult_ref,
        energy_ref,
        proj_ref,
        self_hbm,
        rot_ref,
        dens_ref,
        keep_ref,
        give_ref,
        flat_ref,
        rows_ref,
        self_ref,
        sem,
    ):
        fetch = pltpu.make_async_copy(self_hbm, self_ref, sem)
        fetch.start()
        weight = mult_ref[0].astype(F32)
        shift = lax.axis_index("freq")
        lane = lax.broadcasted_iota(jnp.int32, (n, LANES), 1)
        masks = [(lane >= n * j) & (lane < n * (j + 1)) for j in range(WIDE)]
        energy = energy_ref[...]
        pt = (proj_ref[0, 0], proj_ref[0, 1])
        step = math.pi * thermal_level

        def spread(x):
            tail = jnp.zeros((LANES - WIDE * n, LANES), F32)
            return jnp.concatenate([x] * WIDE + [tail], axis=0).T

        p3 = (spread(pt[0]), spread(pt[1]))
        energy_col = jnp.broadcast_to(energy, (LANES, LANES)).T
        rot = rot_ref[...]
        pt_both = jnp.concatenate([pt[0], pt[1]], axis=1)
        rot_t = rot.T
        turned = mm3(rot_t, pt_both, low(pt_both))
        left = jnp.concatenate([pt_both, turned], axis=0)
        rot_wide = jnp.concatenate([rot] * WIDE + [jnp.zeros((n, LANES - WIDE * n), F32)], axis=1)
        zero = jnp.zeros((LANES, LANES), F32)

        def rot_form(w):
            b = blocks(w, masks)
            return jnp.concatenate(
                [jnp.concatenate([b, zero], axis=1), jnp.concatenate([zero, b], axis=1)], axis=0
            )

        lane_row = lax.broadcasted_iota(jnp.int32, (1, LANES), 1)
        block_of = jnp.where(lane_row >= 2 * n, 2, jnp.where(lane_row >= n, 1, 0))

        gp = []
        for g in range(groups):
            slot = block_of + WIDE * g
            pole = (2 * (slot * pole_stride + shift) + 1).astype(F32) * step
            inv = 1.0 / (pole * pole + energy_col * energy_col)
            br = -energy_col * inv
            bi = -pole * inv
            gp.append((br * p3[0] - bi * p3[1], br * p3[1] + bi * p3[0]))

        big = []
        for g in range(groups):
            xr, xi = gp[g]

            def form(r, i):
                return jnp.concatenate(
                    [jnp.concatenate([r, i], axis=1), jnp.concatenate([i, -r], axis=1)], axis=0
                )

            big.append(mm3(left, form(xr, xi), form(low(xr), low(xi))))
        stacked = jnp.concatenate(big, axis=0)
        right = mm3(stacked, rot_form(rot_wide), rot_form(low(rot_wide)))
        small_right = [right[2 * n * g : 2 * n * g + n] for g in range(groups)]
        both_right = [right[2 * n * g + n : 2 * n * (g + 1)] for g in range(groups)]

        fetch.wait()
        sig = []
        pad = jnp.zeros((n, LANES - WIDE * n), F32)
        none = jnp.zeros((n, n), F32)
        for g in range(groups):
            halves = []
            for c in range(2):
                parts = []
                for j in range(WIDE):
                    q = WIDE * g + j
                    parts.append(self_ref[q, c] if q < pole_total else none)
                halves.append(jnp.concatenate(parts + [pad], axis=1))
            sig.append(jnp.concatenate(halves, axis=1))

        first = [mm3(big[g], *block_weights(sig[g], masks)) for g in range(groups)]
        a1 = [f[:n] for f in first]
        a1_left = [f[n:] for f in first]
        a2 = [mm3(a1[g], *block_weights(a1[g], masks)) for g in range(groups)]
        total = []
        for g in range(groups):
            w = block_weights(a2[g], masks)
            a34 = mm3(jnp.concatenate([a1[g], a2[g]], axis=0), *w)
            a34 = a34[:n] + a34[n:]
            total.append(a1[g] + a2[g] + a34 + mm3(a34, *w))
        last = [
            mm3(jnp.concatenate([sig[g], a1_left[g]], axis=0), *block_weights(total[g], masks))
            for g in range(groups)
        ]
        dress = [sig[g] + last[g][:n] for g in range(groups)]

        acc = None
        for g in range(groups):
            xr, xi = gp[g]
            w = mm3(jnp.concatenate([xr, xi], axis=1), *block_weights(dress[g], masks))
            res, ims = [], []
            for j in range(WIDE):
                q = WIDE * g + j
                pole = (2 * (q * pole_stride + shift) + 1).astype(F32) * step
                inv = 1.0 / (pole * pole + energy * energy)
                br = -energy * inv
                bi = -pole * inv
                res.append(pt[0] * br + pt[1] * bi)
                ims.append(pt[0] * bi - pt[1] * br)
            tail = jnp.zeros((LANES - WIDE * n, LANES), F32)
            re = jnp.concatenate(res + [tail], axis=0)
            im = jnp.concatenate(ims + [tail], axis=0)

            def form(r, i):
                return jnp.concatenate(
                    [jnp.concatenate([r, i], axis=1), jnp.concatenate([-i, r], axis=1)], axis=0
                )

            part = mm3(w, form(re, im), form(low(re), low(im)))
            acc = part if acc is None else acc + part
        er = acc[:, :LANES]
        ei = acc[:, LANES:]
        row = lax.broadcasted_iota(jnp.int32, (LANES, LANES), 0)
        col = lax.broadcasted_iota(jnp.int32, (LANES, LANES), 1)
        scale = weight * thermal_level
        dens_ref[...] = scale * jnp.where(row <= col, er + er.T, ei - ei.T)

        outs = []
        for g in range(groups):
            out = both_right[g] + mm3(
                a1_left[g] + last[g][n:], *block_weights(small_right[g], masks)
            )
            out = weight * out
            outs.append(jnp.concatenate([out[:, :LANES], out[:, LANES:]], axis=0))
        spare = LANES - WIDE * n
        wide_lane = lax.broadcasted_iota(jnp.int32, (2 * n, LANES), 1)
        for g in range(groups - 1):
            moved = pltpu.roll(outs[-1], LANES - spare * (g + 1), 1)
            flat_ref[2 * n * g : 2 * n * (g + 1), :] = jnp.where(
                wide_lane < WIDE * n, outs[g], moved
            )
        rows = 2 * n * (groups - 1)
        flat_ref[rows:, :] = jnp.zeros((flat_ref.shape[0] - rows, LANES), F32)
        for d in range(rows_ref.shape[0]):
            rows_ref[d, 0:USED, :] = flat_ref[USED * d : USED * (d + 1), :]
            rows_ref[d, USED:PIECE, :] = jnp.broadcast_to(weight, (PIECE - USED, LANES))
        core = lax.axis_index("ka") % 2
        for r in range(keep_ref.shape[0]):
            keep_ref[r] = rows_ref[2 * r + core]
            give_ref[r] = rows_ref[2 * r + 1 - core]

    return kernel


def split_kernel(orb_ref, high_ref, other_ref):
    bands = 2 * orb_ref.shape[2]
    slabs = orb_ref.shape[3]
    flat = orb_ref.reshape(bands * slabs, LANES)
    base = pl.program_id(0) * slabs
    for s in range(slabs):
        x = flat[pl.ds(s, bands, stride=slabs), :]
        h = x.astype(BF16)
        high_ref[base + s] = h
        other_ref[base + s] = 2.0 * x - h.astype(F32)


def slab_kernel(mine_ref, theirs_ref, high_ref, other_ref, out_ref):
    packed = mine_ref[...] + theirs_ref[...]
    packed_t = packed.T
    row = lax.broadcasted_iota(jnp.int32, packed.shape, 0)
    col = lax.broadcasted_iota(jnp.int32, packed.shape, 1)
    re = jnp.where(row <= col, packed, packed_t)
    im = jnp.where(row > col, packed, jnp.where(row < col, -packed_t, 0.0))
    full = jnp.concatenate(
        [jnp.concatenate([re, -im], axis=1), jnp.concatenate([im, re], axis=1)], axis=0
    )
    high = full.astype(BF16)
    rest = (full - high.astype(F32)).astype(BF16)
    slabs = high_ref.shape[0]
    for s in range(0, slabs, 2):
        cols = jnp.concatenate([high_ref[s], high_ref[s + 1]], axis=1)
        prod = mm(high, cols) + mm(rest, cols)
        for t in range(2):
            rho = jnp.sum(
                other_ref[s + t] * prod[:, LANES * t : LANES * (t + 1)], axis=0, keepdims=True
            )
            out_ref[s + t : s + t + 1, :] = rho


def pack_kernel(owner_ref, local_ref, charge_ref, out_ref):
    sums = jnp.sum(local_ref[...], axis=0)
    inverse = 1.0 / sums[USED : USED + 1, :]
    sums = sums * inverse
    for d in range(out_ref.shape[0]):
        out_ref[d] = sums
    for s in range(charge_ref.shape[0]):
        own = owner_ref[s]
        out_ref[own // 2, pl.ds(USED + own % 2, 1), :] = charge_ref[s : s + 1, :] * inverse


def unpack_kernel(pole_total, orbital_count):
    n = orbital_count

    def kernel(mine_ref, theirs_ref, green_ref, charge_ref, rows_ref, flat_ref):
        core = lax.axis_index("ka") % 2
        pieces = mine_ref.shape[0]
        total = None
        for r in range(pieces):
            rows_ref[2 * r + core] = mine_ref[r]
            rows_ref[2 * r + 1 - core] = theirs_ref[r]
            both = mine_ref[r, USED : USED + 2, :] + theirs_ref[r, USED : USED + 2, :]
            total = both if total is None else total + both
        charge_ref[...] = jnp.where(core == 0, total[0:1], total[1:2])
        for d in range(2 * pieces):
            flat_ref[USED * d : USED * (d + 1), :] = rows_ref[d, 0:USED, :]
        for q in range(pole_total - 1):
            g, j = divmod(q, WIDE)
            for c in range(2):
                base = n * (2 * g + c)
                green_ref[q, c] = flat_ref[base : base + n, n * j : n * (j + 1)]
        spare = LANES - WIDE * n
        for c in range(2):
            parts = [
                flat_ref[n * (2 * g + c) : n * (2 * g + c + 1), WIDE * n :]
                for g in range(n // spare)
            ]
            green_ref[pole_total - 1, c] = jnp.concatenate(parts, axis=1)

    return kernel


def whole(memory=None):
    return pl.BlockSpec(memory_space=memory or pltpu.VMEM)


def held(x):
    return pltpu.with_memory_space_constraint(x, pltpu.VMEM)


def far(x):
    return pltpu.with_memory_space_constraint(x, pltpu.HBM)


def local(energy, projector, self_energy, multiplicity, orbitals, owner, rotation):
    pole_total = self_energy.shape[0]
    n = self_energy.shape[2]
    slabs = orbitals.shape[3]
    peers = lax.axis_size("ka")
    poles = lax.axis_size("freq")
    bands = projector.shape[2]
    thermal_level = 0.25 / (pole_total * poles)
    groups = -(-pole_total // WIDE)
    flat_rows = USED * peers
    assert flat_rows >= 2 * n * (groups - 1) and bands == LANES
    assert pole_total == WIDE * (groups - 1) + 1 and (LANES - WIDE * n) * (groups - 1) == n
    chips = peers // 2

    dens, keep, give = pl.pallas_call(
        green_kernel(pole_total, n, poles, thermal_level),
        out_shape=(
            pltpu.VMEM((bands, bands), F32),
            pltpu.VMEM((chips, PIECE, LANES), F32),
            pltpu.VMEM((chips, PIECE, LANES), F32),
        ),
        in_specs=[whole(pltpu.SMEM), whole(), whole(), whole(pl.ANY), whole()],
        out_specs=(whole(), whole(), whole()),
        scratch_shapes=[
            pltpu.VMEM((flat_rows, LANES), F32),
            pltpu.VMEM((peers, PIECE, LANES), F32),
            pltpu.VMEM(self_energy.shape, F32),
            pltpu.SemaphoreType.DMA,
        ],
        compiler_params=pltpu.CompilerParams(vmem_limit_bytes=20 << 20),
        name="green",
    )(
        multiplicity,
        far(energy),
        far(jnp.swapaxes(projector, 2, 3)),
        far(self_energy),
        far(rotation),
    )

    def swapped(x, axis, flip):
        return lax.ppermute(x, axis, [(i, i ^ flip) for i in range(lax.axis_size(axis))])

    def across_chips(x):
        same_core = [[2 * i + c for i in range(chips)] for c in range(2)]
        return lax.all_to_all(x, "ka", 0, 0, axis_index_groups=same_core, tiled=True)

    given = swapped(give, "ka", 1)
    arrived = [swapped(dens, "freq", d) for d in range(1, 4)]
    rows = keep + given
    rows_in = across_chips(rows)
    dens = (dens + arrived[0]) + (arrived[1] + arrived[2])
    theirs = swapped(dens, "freq", 4)

    step = 8
    high, other = pl.pallas_call(
        split_kernel,
        grid=(slabs // step,),
        in_specs=[pl.BlockSpec((1, 2, bands, step, LANES), lambda i: (0, 0, 0, i, 0))],
        out_specs=(whole(), whole()),
        out_shape=(
            pltpu.VMEM((slabs, 2 * bands, LANES), BF16),
            pltpu.VMEM((slabs, 2 * bands, LANES), F32),
        ),
        compiler_params=pltpu.CompilerParams(vmem_limit_bytes=8 << 20),
        name="split",
    )(far(orbitals))
    rho = pl.pallas_call(
        slab_kernel,
        out_shape=pltpu.VMEM((slabs, LANES), F32),
        in_specs=[whole()] * 4,
        out_specs=whole(),
        compiler_params=pltpu.CompilerParams(vmem_limit_bytes=8 << 20),
        name="slab",
    )(*[held(x) for x in (dens, theirs, high, other)])
    sends = pl.pallas_call(
        pack_kernel,
        out_shape=pltpu.VMEM((chips, PIECE, LANES), F32),
        in_specs=[whole(pltpu.SMEM), whole(), whole()],
        out_specs=whole(),
        compiler_params=pltpu.CompilerParams(vmem_limit_bytes=4 << 20),
        name="pack",
    )(owner, held(rows_in), held(rho))
    back = across_chips(sends)
    across = swapped(back, "ka", 1)

    local_green, slab = pl.pallas_call(
        unpack_kernel(pole_total, n),
        out_shape=(
            jax.ShapeDtypeStruct((pole_total, 2, n, n), F32),
            jax.ShapeDtypeStruct((1, LANES), F32),
        ),
        in_specs=[whole(), whole()],
        out_specs=(whole(), whole()),
        scratch_shapes=[
            pltpu.VMEM((peers, PIECE, LANES), F32),
            pltpu.VMEM((flat_rows, LANES), F32),
        ],
        compiler_params=pltpu.CompilerParams(vmem_limit_bytes=6 << 20),
        name="unpack",
    )(held(back), held(across))
    return (local_green, slab)


def solution(mesh):
    in_specs = (
        P("ka", None),
        P("ka", None, None, None),
        P("freq", None, None, None),
        P("ka"),
        P("ka", None, None, None, "freq"),
        P(),
        P(),
    )
    out_specs = (P("freq", None, None, None), P("ka", "freq"))
    return jax.shard_map(local, mesh=mesh, in_specs=in_specs, out_specs=out_specs, check_vma=False)
```

```python
import math

import jax
import jax.numpy as jnp
from jax import lax
from jax.experimental import pallas as pl
from jax.experimental.pallas import tpu as pltpu
from jax.sharding import PartitionSpec as P


F32 = jnp.float32
BF16 = jnp.bfloat16
LANES = 128
WIDE = 3
PIECE = 16
USED = 13


def low(x):
    return x - x.astype(BF16).astype(F32)


def mm(a, b):
    return jnp.dot(a, b, preferred_element_type=F32)


def mm3(a, b, b_low):
    rows = a.shape[0]
    both = mm(jnp.concatenate([a, low(a)], axis=0), b)
    return both[:rows] + both[rows:] + mm(a, b_low)


def blocks(wide, masks):
    n = wide.shape[0]
    rows = [jnp.where(m, wide, 0.0) for m in masks]
    rows.append(jnp.zeros((LANES - WIDE * n, LANES), F32))
    return jnp.concatenate(rows, axis=0)


def block_weights(wide, masks):
    def form(w):
        re = blocks(w[:, :LANES], masks)
        im = blocks(w[:, LANES:], masks)
        return jnp.concatenate(
            [jnp.concatenate([re, im], axis=1), jnp.concatenate([-im, re], axis=1)], axis=0
        )

    return form(wide), form(low(wide))


def green_kernel(pole_total, orbital_count, pole_stride, thermal_level):
    groups = -(-pole_total // WIDE)
    n = orbital_count

    def kernel(
        mult_ref,
        energy_ref,
        proj_ref,
        self_hbm,
        rot_ref,
        dens_ref,
        keep_ref,
        give_ref,
        flat_ref,
        rows_ref,
        self_ref,
        sem,
    ):
        fetch = pltpu.make_async_copy(self_hbm, self_ref, sem)
        fetch.start()
        weight = mult_ref[0].astype(F32)
        shift = lax.axis_index("freq")
        lane = lax.broadcasted_iota(jnp.int32, (n, LANES), 1)
        masks = [(lane >= n * j) & (lane < n * (j + 1)) for j in range(WIDE)]
        energy = energy_ref[...]
        pt = (proj_ref[0, 0], proj_ref[0, 1])
        step = math.pi * thermal_level

        def spread(x):
            tail = jnp.zeros((LANES - WIDE * n, LANES), F32)
            return jnp.concatenate([x] * WIDE + [tail], axis=0).T

        p3 = (spread(pt[0]), spread(pt[1]))
        energy_col = jnp.broadcast_to(energy, (LANES, LANES)).T
        rot = rot_ref[...]
        pt_both = jnp.concatenate([pt[0], pt[1]], axis=1)
        rot_t = rot.T
        turned = mm3(rot_t, pt_both, low(pt_both))
        left = jnp.concatenate([pt_both, turned], axis=0)
        rot_wide = jnp.concatenate([rot] * WIDE + [jnp.zeros((n, LANES - WIDE * n), F32)], axis=1)
        zero = jnp.zeros((LANES, LANES), F32)

        def rot_form(w):
            b = blocks(w, masks)
            return jnp.concatenate(
                [jnp.concatenate([b, zero], axis=1), jnp.concatenate([zero, b], axis=1)], axis=0
            )

        lane_row = lax.broadcasted_iota(jnp.int32, (1, LANES), 1)
        block_of = jnp.where(lane_row >= 2 * n, 2, jnp.where(lane_row >= n, 1, 0))

        gp = []
        for g in range(groups):
            slot = block_of + WIDE * g
            pole = (2 * (slot * pole_stride + shift) + 1).astype(F32) * step
            inv = 1.0 / (pole * pole + energy_col * energy_col)
            br = -energy_col * inv
            bi = -pole * inv
            gp.append((br * p3[0] - bi * p3[1], br * p3[1] + bi * p3[0]))

        big = []
        for g in range(groups):
            xr, xi = gp[g]

            def form(r, i):
                return jnp.concatenate(
                    [jnp.concatenate([r, i], axis=1), jnp.concatenate([i, -r], axis=1)], axis=0
                )

            big.append(mm3(left, form(xr, xi), form(low(xr), low(xi))))
        stacked = jnp.concatenate(big, axis=0)
        right = mm3(stacked, rot_form(rot_wide), rot_form(low(rot_wide)))
        small_right = [right[2 * n * g : 2 * n * g + n] for g in range(groups)]
        both_right = [right[2 * n * g + n : 2 * n * (g + 1)] for g in range(groups)]

        fetch.wait()
        sig = []
        pad = jnp.zeros((n, LANES - WIDE * n), F32)
        none = jnp.zeros((n, n), F32)
        for g in range(groups):
            halves = []
            for c in range(2):
                parts = []
                for j in range(WIDE):
                    q = WIDE * g + j
                    parts.append(self_ref[q, c] if q < pole_total else none)
                halves.append(jnp.concatenate(parts + [pad], axis=1))
            sig.append(jnp.concatenate(halves, axis=1))

        first = [mm3(big[g], *block_weights(sig[g], masks)) for g in range(groups)]
        a1 = [f[:n] for f in first]
        a1_left = [f[n:] for f in first]
        a2 = [mm3(a1[g], *block_weights(a1[g], masks)) for g in range(groups)]
        total = []
        for g in range(groups):
            w = block_weights(a2[g], masks)
            a34 = mm3(jnp.concatenate([a1[g], a2[g]], axis=0), *w)
            a34 = a34[:n] + a34[n:]
            total.append(a1[g] + a2[g] + a34 + mm3(a34, *w))
        last = [
            mm3(jnp.concatenate([sig[g], a1_left[g]], axis=0), *block_weights(total[g], masks))
            for g in range(groups)
        ]
        dress = [sig[g] + last[g][:n] for g in range(groups)]

        outs = []
        for g in range(groups):
            out = both_right[g] + mm3(
                a1_left[g] + last[g][n:], *block_weights(small_right[g], masks)
            )
            out = weight * out
            outs.append(jnp.concatenate([out[:, :LANES], out[:, LANES:]], axis=0))
        spare = LANES - WIDE * n
        wide_lane = lax.broadcasted_iota(jnp.int32, (2 * n, LANES), 1)
        for g in range(groups - 1):
            moved = pltpu.roll(outs[-1], LANES - spare * (g + 1), 1)
            flat_ref[2 * n * g : 2 * n * (g + 1), :] = jnp.where(
                wide_lane < WIDE * n, outs[g], moved
            )
        rows = 2 * n * (groups - 1)
        flat_ref[rows:, :] = jnp.zeros((flat_ref.shape[0] - rows, LANES), F32)
        for d in range(rows_ref.shape[0]):
            rows_ref[d, 0:USED, :] = flat_ref[USED * d : USED * (d + 1), :]
            rows_ref[d, USED:PIECE, :] = jnp.broadcast_to(weight, (PIECE - USED, LANES))
        core = lax.axis_index("ka") % 2
        for r in range(keep_ref.shape[0]):
            keep_ref[r] = rows_ref[2 * r + core]
            give_ref[r] = rows_ref[2 * r + 1 - core]

        acc = None
        for g in range(groups):
            xr, xi = gp[g]
            w = mm3(jnp.concatenate([xr, xi], axis=1), *block_weights(dress[g], masks))
            res, ims = [], []
            for j in range(WIDE):
                q = WIDE * g + j
                pole = (2 * (q * pole_stride + shift) + 1).astype(F32) * step
                inv = 1.0 / (pole * pole + energy * energy)
                br = -energy * inv
                bi = -pole * inv
                res.append(pt[0] * br + pt[1] * bi)
                ims.append(pt[0] * bi - pt[1] * br)
            tail = jnp.zeros((LANES - WIDE * n, LANES), F32)
            re = jnp.concatenate(res + [tail], axis=0)
            im = jnp.concatenate(ims + [tail], axis=0)

            def form(r, i):
                return jnp.concatenate(
                    [jnp.concatenate([r, i], axis=1), jnp.concatenate([-i, r], axis=1)], axis=0
                )

            part = mm3(w, form(re, im), form(low(re), low(im)))
            acc = part if acc is None else acc + part
        er = acc[:, :LANES]
        ei = acc[:, LANES:]
        row = lax.broadcasted_iota(jnp.int32, (LANES, LANES), 0)
        col = lax.broadcasted_iota(jnp.int32, (LANES, LANES), 1)
        scale = weight * thermal_level
        dens_ref[...] = scale * jnp.where(row <= col, er + er.T, ei - ei.T)

    return kernel


def split_kernel(owner_ref, orb_ref, high_ref, other_ref):
    bands = 2 * orb_ref.shape[2]
    slabs = orb_ref.shape[3]
    flat = orb_ref.reshape(bands * slabs, LANES)
    base = pl.program_id(0) * slabs
    for s in range(slabs):
        x = flat[pl.ds(s, bands, stride=slabs), :]
        h = x.astype(BF16)
        own = owner_ref[base + s]
        high_ref[own] = h
        other_ref[own] = 2.0 * x - h.astype(F32)


def slab_kernel(mine_ref, theirs_ref, high_ref, other_ref, out_ref):
    packed = mine_ref[...] + theirs_ref[...]
    packed_t = packed.T
    row = lax.broadcasted_iota(jnp.int32, packed.shape, 0)
    col = lax.broadcasted_iota(jnp.int32, packed.shape, 1)
    re = jnp.where(row <= col, packed, packed_t)
    im = jnp.where(row > col, packed, jnp.where(row < col, -packed_t, 0.0))
    full = jnp.concatenate(
        [jnp.concatenate([re, -im], axis=1), jnp.concatenate([im, re], axis=1)], axis=0
    )
    high = full.astype(BF16)
    rest = (full - high.astype(F32)).astype(BF16)
    slabs = high_ref.shape[0]
    for s in range(0, slabs, 2):
        cols = jnp.concatenate([high_ref[s], high_ref[s + 1]], axis=1)
        prod = mm(high, cols) + mm(rest, cols)
        for t in range(2):
            rho = jnp.sum(
                other_ref[s + t] * prod[:, LANES * t : LANES * (t + 1)], axis=0, keepdims=True
            )
            out_ref[s + t : s + t + 1, :] = rho


def pack_kernel(local_ref, charge_ref, out_ref):
    sums = jnp.sum(local_ref[...], axis=0)
    inverse = 1.0 / sums[USED : USED + 1, :]
    sums = sums * inverse
    charge = charge_ref[...] * inverse
    for d in range(out_ref.shape[0]):
        out_ref[d] = sums
        out_ref[d, USED : USED + 2, :] = charge[2 * d : 2 * d + 2]


def unpack_kernel(pole_total, orbital_count):
    n = orbital_count

    def kernel(mine_ref, theirs_ref, green_ref, charge_ref, rows_ref, flat_ref):
        core = lax.axis_index("ka") % 2
        pieces = mine_ref.shape[0]
        total = None
        for r in range(pieces):
            rows_ref[2 * r + core] = mine_ref[r]
            rows_ref[2 * r + 1 - core] = theirs_ref[r]
            both = mine_ref[r, USED : USED + 2, :] + theirs_ref[r, USED : USED + 2, :]
            total = both if total is None else total + both
        charge_ref[...] = jnp.where(core == 0, total[0:1], total[1:2])
        for d in range(2 * pieces):
            flat_ref[USED * d : USED * (d + 1), :] = rows_ref[d, 0:USED, :]
        for q in range(pole_total - 1):
            g, j = divmod(q, WIDE)
            for c in range(2):
                base = n * (2 * g + c)
                green_ref[q, c] = flat_ref[base : base + n, n * j : n * (j + 1)]
        spare = LANES - WIDE * n
        for c in range(2):
            parts = [
                flat_ref[n * (2 * g + c) : n * (2 * g + c + 1), WIDE * n :]
                for g in range(n // spare)
            ]
            green_ref[pole_total - 1, c] = jnp.concatenate(parts, axis=1)

    return kernel


def whole(memory=None):
    return pl.BlockSpec(memory_space=memory or pltpu.VMEM)


def held(x):
    return pltpu.with_memory_space_constraint(x, pltpu.VMEM)


def far(x):
    return pltpu.with_memory_space_constraint(x, pltpu.HBM)


def local(energy, projector, self_energy, multiplicity, orbitals, owner, rotation):
    pole_total = self_energy.shape[0]
    n = self_energy.shape[2]
    slabs = orbitals.shape[3]
    peers = lax.axis_size("ka")
    poles = lax.axis_size("freq")
    bands = projector.shape[2]
    thermal_level = 0.25 / (pole_total * poles)
    groups = -(-pole_total // WIDE)
    flat_rows = USED * peers
    assert flat_rows >= 2 * n * (groups - 1) and bands == LANES
    assert pole_total == WIDE * (groups - 1) + 1 and (LANES - WIDE * n) * (groups - 1) == n
    chips = peers // 2

    dens, keep, give = pl.pallas_call(
        green_kernel(pole_total, n, poles, thermal_level),
        out_shape=(
            pltpu.VMEM((bands, bands), F32),
            pltpu.VMEM((chips, PIECE, LANES), F32),
            pltpu.VMEM((chips, PIECE, LANES), F32),
        ),
        in_specs=[whole(pltpu.SMEM), whole(), whole(), whole(pl.ANY), whole()],
        out_specs=(whole(), whole(), whole()),
        scratch_shapes=[
            pltpu.VMEM((flat_rows, LANES), F32),
            pltpu.VMEM((peers, PIECE, LANES), F32),
            pltpu.VMEM(self_energy.shape, F32),
            pltpu.SemaphoreType.DMA,
        ],
        compiler_params=pltpu.CompilerParams(vmem_limit_bytes=20 << 20),
        name="green",
    )(
        multiplicity,
        far(energy),
        far(jnp.swapaxes(projector, 2, 3)),
        far(self_energy),
        far(rotation),
    )

    def swapped(x, axis, flip):
        return lax.ppermute(x, axis, [(i, i ^ flip) for i in range(lax.axis_size(axis))])

    def across_chips(x):
        same_core = [[2 * i + c for i in range(chips)] for c in range(2)]
        return lax.all_to_all(x, "ka", 0, 0, axis_index_groups=same_core, tiled=True)

    given = swapped(give, "ka", 1)
    arrived = [swapped(dens, "freq", d) for d in (1, 3, 2)]
    rows = keep + given
    rows_in = across_chips(rows)
    dens = (dens + arrived[0]) + (arrived[1] + arrived[2])
    theirs = swapped(dens, "freq", 4)

    step = 8
    high, other = pl.pallas_call(
        split_kernel,
        grid=(slabs // step,),
        in_specs=[
            whole(pltpu.SMEM),
            pl.BlockSpec((1, 2, bands, step, LANES), lambda i: (0, 0, 0, i, 0)),
        ],
        out_specs=(whole(), whole()),
        out_shape=(
            pltpu.VMEM((slabs, 2 * bands, LANES), BF16),
            pltpu.VMEM((slabs, 2 * bands, LANES), F32),
        ),
        compiler_params=pltpu.CompilerParams(vmem_limit_bytes=8 << 20),
        name="split",
    )(far(owner), far(orbitals))
    rho = pl.pallas_call(
        slab_kernel,
        out_shape=pltpu.VMEM((slabs, LANES), F32),
        in_specs=[whole()] * 4,
        out_specs=whole(),
        compiler_params=pltpu.CompilerParams(vmem_limit_bytes=8 << 20),
        name="slab",
    )(*[held(x) for x in (dens, theirs, high, other)])
    sends = pl.pallas_call(
        pack_kernel,
        out_shape=pltpu.VMEM((chips, PIECE, LANES), F32),
        in_specs=[whole(), whole()],
        out_specs=whole(),
        compiler_params=pltpu.CompilerParams(vmem_limit_bytes=4 << 20),
        name="pack",
    )(held(rows_in), held(rho))
    back = across_chips(sends)
    across = swapped(back, "ka", 1)

    local_green, slab = pl.pallas_call(
        unpack_kernel(pole_total, n),
        out_shape=(
            jax.ShapeDtypeStruct((pole_total, 2, n, n), F32),
            jax.ShapeDtypeStruct((1, LANES), F32),
        ),
        in_specs=[whole(), whole()],
        out_specs=(whole(), whole()),
        scratch_shapes=[
            pltpu.VMEM((peers, PIECE, LANES), F32),
            pltpu.VMEM((flat_rows, LANES), F32),
        ],
        compiler_params=pltpu.CompilerParams(vmem_limit_bytes=6 << 20),
        name="unpack",
    )(held(back), held(across))
    return (local_green, slab)


def solution(mesh):
    in_specs = (
        P("ka", None),
        P("ka", None, None, None),
        P("freq", None, None, None),
        P("ka"),
        P("ka", None, None, None, "freq"),
        P(),
        P(),
    )
    out_specs = (P("freq", None, None, None), P("ka", "freq"))
    return jax.shard_map(local, mesh=mesh, in_specs=in_specs, out_specs=out_specs, check_vma=False)
```
